256 devices in a mesh: dp: 32 (over z, x), patch: 8 (over y, core).
Axes of the slice: x: 4, y: 4, z: 8, core: 2. Of those that a mesh axis runs over, the one named last changes fastest.
Arguments:
- token_ids: int32 [512], replicated, may hold values from 0 to 31999
- parents: int32 [512], replicated, may hold values from 0 to 3
- embedding: bfloat16 [32000, 1024], P('dp'), may hold values from -6 to 6
- self_gain: bfloat16 [1024], replicated, may hold values from 0.25 to 1.75
- query_weight: bfloat16 [1024, 1024], P(None, 'patch'), may hold values from -0.1875 to 0.1875
- key_weight: bfloat16 [1024, 1024], P(None, 'patch'), may hold values from -0.1875 to 0.1875
- value_weight: bfloat16 [1024, 1024], P(None, 'patch'), may hold values from -0.1875 to 0.1875
- output_weight: bfloat16 [1024, 1024], P('patch'), may hold values from -0.75 to 0.75
- past_keys: bfloat16 [512, 128, 1024], P('dp', None, 'patch'), may hold values from -200 to 200
- past_values: bfloat16 [512, 128, 1024], P('dp', None, 'patch'), may hold values from -6 to 6
- cross_gain: bfloat16 [1024], replicated, may hold values from 0.25 to 1.75
- cross_query: bfloat16 [1024, 1024], replicated, may hold values from -0.1875 to 0.1875
- cross_output: bfloat16 [1024, 1024], replicated, may hold values from -0.75 to 0.75
- image_keys: bfloat16 [32, 16, 256, 1024], P('dp', None, 'patch'), may hold values from -260 to 260
- image_values: bfloat16 [32, 16, 256, 1024], P('dp', None, 'patch'), may hold values from -6 to 6
Outputs:
- hidden: bfloat16 [512, 1024], P('dp')
- new_keys: bfloat16 [512, 1024], P('dp', 'patch')
- new_values: bfloat16 [512, 1024], P('dp', 'patch')
The draws below stay inside these ranges and needn't reach their ends.
Inputs may be any that keep to these rules, and one draw needn't show every extreme that they name: `parents`: a beam of the row's own image.
All inputs are finite; a program needn't handle non-finite values.
Results may differ from the reference program's by a relative error of at most 0.019.
The reference program's roundings to bfloat16 on the way count: a program that leaves them out, or rounds other values in their place, can miss the bound.
Values may be sent and summed in bfloat16 or wider, within the bound.
A program may use at most 64 MiB of HBM per device.

```python
import math
import jax
import jax.numpy as jnp
import numpy as np
from jax import lax

D = 1024
HEADS = 16
PATCHES = 1024
VOCAB = 32000
BEAMS = 4
LEN = 128
IMG_DEV = 16
HD = 64
ROWS = 512
N_DP = 32


def loud_sample(key, array_shape, spread):
    key_base = jax.random.fold_in(key, 0)
    sample = spread * jnp.clip(jax.random.normal(key_base, array_shape, jnp.float32), -6.0, 6.0)
    return sample


def draw_past_keys(key, part):
    return loud_sample(jax.random.fold_in(key, 11), (ROWS, LEN, D), 1.5).astype(jnp.bfloat16)


def draw_image_keys(key, part):
    return loud_sample(jax.random.fold_in(key, 23), (N_DP, IMG_DEV, PATCHES // BEAMS, D), 2.0).astype(jnp.bfloat16)


def plant(values, own_key, low, top_value):
    dims = values.shape
    place = [jax.random.randint(jax.random.fold_in(own_key, axis), (), 0, dims[axis]) for axis in range(len(dims))]
    values = values.at[tuple(place)].set(low)
    longest = dims.index(max(dims))
    place[longest] = (place[longest] + 1) % dims[longest]
    return values.at[tuple(place)].set(top_value)


def steps_of(key, shape, cuts, smallest, high):
    loudness, own = 1.0, jax.random.fold_in(key, 6)
    for axis_at, parts in cuts:
        steps = jnp.exp(jax.random.uniform(jax.random.fold_in(own, axis_at), (parts,), jnp.float32, smallest / len(cuts), high / len(cuts)))
        loudness = loudness * jnp.repeat(steps, shape[axis_at] // parts).reshape([-1 if axis == axis_at else 1 for axis in range(len(shape))])
    return loudness


def rank_bounds(amount, lean):
    weights = [(1 << 20) // math.isqrt(standing ** lean) + 1 for standing in range(1, amount + 1)]
    width = 1 + sum(weights) // (1 << 30)
    return np.cumsum(np.array([max(1, weight // width) for weight in weights]))


def ranked_ids(key, dims, number_of, skew):
    table = rank_bounds(number_of, skew)
    lot = jax.random.randint(jax.random.fold_in(key, 1), dims, 0, int(table[number_of - 1]))
    standing = jnp.searchsorted(jnp.asarray(table, jnp.int32), lot, side="right")
    return jax.random.permutation(jax.random.fold_in(key, 2), number_of)[standing].astype(jnp.int32)


def centred(stream_key, shape, scale, limit, cuts=(), kind=jnp.bfloat16):
    values = scale * jax.random.normal(stream_key, shape, jnp.float32)
    if cuts:
        values = values * steps_of(stream_key, shape, cuts, -0.22, 0.18)
    return jnp.clip(values, -limit, limit).astype(kind)


def setup_inputs(seed: int = 0) -> dict:
    keys = jax.random.split(jax.random.key(seed), 16)
    token_ids = plant(ranked_ids(keys[0], (ROWS,), VOCAB, 2), jax.random.fold_in(keys[0], 3), 0, VOCAB - 1).astype(jnp.int32)
    parents = plant(jax.random.randint(keys[1], (ROWS,), 0, BEAMS), jax.random.fold_in(keys[1], 1), 0, BEAMS - 1).astype(jnp.int32)
    embedding = centred(keys[2], (VOCAB, D), 1.0, 6.0, ((0, 32),))
    self_gain = jnp.clip(1.0 + 0.15 * jax.random.normal(keys[3], (D,), jnp.float32), 0.25, 1.75).astype(jnp.bfloat16)
    query_weight = centred(keys[4], (D, D), D ** -0.5, 0.1875, ((1, 8),))
    key_weight = centred(keys[5], (D, D), D ** -0.5, 0.1875, ((1, 8),))
    value_weight = centred(keys[6], (D, D), D ** -0.5, 0.1875, ((1, 8),))
    output_weight = centred(keys[7], (D, D), HD ** -0.5, 0.75, ((0, 8),))
    past_keys = draw_past_keys(jax.random.fold_in(keys[15], 71), 0)
    past_values = centred(keys[9], (ROWS, LEN, D), 1.0, 6.0, ((0, 32), (2, 8)))
    cross_gain = jnp.clip(1.0 + 0.15 * jax.random.normal(keys[10], (D,), jnp.float32), 0.25, 1.75).astype(jnp.bfloat16)
    cross_query = centred(keys[11], (D, D), D ** -0.5, 0.1875)
    cross_output = centred(keys[12], (D, D), HD ** -0.5, 0.75)
    image_keys = draw_image_keys(jax.random.fold_in(keys[15], 71), 0)
    image_values = centred(keys[14], (N_DP, IMG_DEV, PATCHES // BEAMS, D), 1.0, 6.0, ((0, 32), (2, 8)))
    return {"token_ids": token_ids, "parents": parents, "embedding": embedding, "self_gain": self_gain, "query_weight": query_weight, "key_weight": key_weight, "value_weight": value_weight, "output_weight": output_weight, "past_keys": past_keys, "past_values": past_values, "cross_gain": cross_gain, "cross_query": cross_query, "cross_output": cross_output, "image_keys": image_keys, "image_values": image_values}


def normalize(inputs, gains):
    factor = lax.rsqrt(lax.optimization_barrier(jnp.mean(inputs * inputs, axis=-1, keepdims=True)) + 1e-06)
    return (inputs * factor * gains.astype(jnp.float32)).astype(jnp.bfloat16)

def soften(scores):
    maxima = lax.optimization_barrier(jnp.max(scores, axis=-1, keepdims=True))
    powers = jnp.exp(scores - maxima)
    totals = lax.optimization_barrier(jnp.sum(powers, axis=-1))
    rounded = lax.optimization_barrier(powers.astype(jnp.bfloat16)).astype(jnp.float32)
    return (rounded, totals)

def reference(token_ids, parents, embedding, self_gain, query_weight, key_weight, value_weight, output_weight, past_keys, past_values, cross_gain, cross_query, cross_output, image_keys, image_values):
    row_count = token_ids.shape[0]
    scaling = 1.0 / HD ** 0.5
    tokens = jnp.take(embedding, token_ids, axis=0).astype(jnp.float32)
    normed = normalize(tokens, self_gain)
    queries = jnp.dot(normed, query_weight, preferred_element_type=jnp.float32).astype(jnp.bfloat16)
    new_keys = jnp.dot(normed, key_weight, preferred_element_type=jnp.float32).astype(jnp.bfloat16)
    new_values = jnp.dot(normed, value_weight, preferred_element_type=jnp.float32).astype(jnp.bfloat16)
    row_index = jnp.arange(row_count, dtype=jnp.int32)
    stride = BEAMS * IMG_DEV
    source = row_index // stride * stride + parents.astype(jnp.int32) * IMG_DEV + row_index % IMG_DEV
    old_keys = jnp.take(past_keys, source, axis=0).astype(jnp.float32).reshape(row_count, LEN, HEADS, HD)
    old_values = jnp.take(past_values, source, axis=0).astype(jnp.float32).reshape(row_count, LEN, HEADS, HD)
    query_heads = queries.astype(jnp.float32).reshape(row_count, HEADS, HD)
    key_heads = new_keys.astype(jnp.float32).reshape(row_count, HEADS, HD)
    value_heads = new_values.astype(jnp.float32).reshape(row_count, HEADS, HD)
    scores = jnp.einsum('rhe,rlhe->rhl', query_heads, old_keys) * scaling
    own_score = lax.optimization_barrier(jnp.sum(query_heads * key_heads, axis=-1))[..., None] * scaling
    rounded, totals = soften(jnp.concatenate([scores, own_score], axis=-1))
    numerators = jnp.einsum('rhl,rlhe->rhe', rounded[..., :LEN], old_values) + rounded[..., LEN:] * value_heads
    self_context = (numerators / totals[..., None]).reshape(row_count, D).astype(jnp.bfloat16)
    middle = tokens + jnp.dot(self_context, output_weight, preferred_element_type=jnp.float32)
    probes = jnp.dot(normalize(middle, cross_gain), cross_query, preferred_element_type=jnp.float32).astype(jnp.bfloat16)
    groups = N_DP // BEAMS
    quarter = PATCHES // BEAMS
    probe_groups = probes.reshape(groups, BEAMS, IMG_DEV, HEADS, HD)
    key_groups = image_keys.reshape(groups, BEAMS, IMG_DEV, quarter, D)
    value_groups = image_values.reshape(groups, BEAMS, IMG_DEV, quarter, D)

    def one_group(pieces):
        probe_here, keys_here, values_here = pieces
        keys_here = jnp.transpose(keys_here.astype(jnp.float32), (1, 0, 2, 3)).reshape(IMG_DEV, PATCHES, HEADS, HD)
        values_here = jnp.transpose(values_here.astype(jnp.float32), (1, 0, 2, 3)).reshape(IMG_DEV, PATCHES, HEADS, HD)
        cross_scores = jnp.einsum('bihe,iphe->bihp', probe_here.astype(jnp.float32), keys_here) * scaling
        weights, sums = soften(cross_scores)
        summed = jnp.einsum('bihp,iphe->bihe', weights, values_here)
        return (summed / sums[..., None]).reshape(BEAMS * IMG_DEV, D).astype(jnp.bfloat16)
    cross_context = lax.map(one_group, (probe_groups, key_groups, value_groups)).reshape(row_count, D)
    hidden = (middle + jnp.dot(cross_context, cross_output, preferred_element_type=jnp.float32)).astype(jnp.bfloat16)
    return (hidden, new_keys, new_values)
```

```python
import jax
import jax.numpy as jnp
from jax import lax
from jax.experimental import pallas as pl
from jax.experimental.pallas import tpu as pltpu
from jax.sharding import PartitionSpec as P

MESH = pl.DeviceIdType.MESH
F32 = jnp.float32
BF16 = jnp.bfloat16

D = 1024
CHUNKS = 8
BEAMS = 4
IMAGES = 16
ROWS = BEAMS * IMAGES
DP = 32
PATCH = 8
PLANE = 32
SLAB = 1000
LEN = 128
SPOTS = 32
NEG = -1e30
NT = (((1,), (1,)), ((), ()))


def dot(a, b):
    return jnp.dot(a, b, preferred_element_type=F32)


def dot_nt(a, b):
    return lax.dot_general(a, b, NT, preferred_element_type=F32)


def tree(parts):
    while len(parts) > 1:
        parts = [a + b for a, b in zip(parts[::2], parts[1::2])] + (
            [parts[-1]] if len(parts) % 2 else []
        )
    return parts[0]


def loop(count, step):
    def body(k, carry):
        step(k)
        return carry

    lax.fori_loop(1, count, body, 0)


def split_heads(x):
    lane = lax.broadcasted_iota(jnp.int32, x.shape, 1)
    low = jnp.where(lane < 64, x, 0.0)
    high = jnp.where(lane < 64, 0.0, x)
    return jnp.concatenate([low, high], axis=0).astype(BF16)


def join_heads(x):
    half = x.shape[0] // 2
    lane = lax.broadcasted_iota(jnp.int32, (half, 128), 1)
    return jnp.where(lane < 64, x[:half], x[half:])


def kernel(
    ids_ref,
    parents_ref,
    emb_ref,
    sgain_ref,
    wq_ref,
    wk_ref,
    wv_ref,
    wo_ref,
    pk_ref,
    pv_ref,
    cgain_ref,
    cq_ref,
    co_ref,
    ik_ref,
    iv_ref,
    hidden_ref,
    newk_ref,
    newv_ref,
    emb,
    wqkv,
    wo,
    pk,
    pv,
    cq,
    co,
    ik,
    iv,
    owned,
    r1,
    tokc,
    r2,
    tokf,
    masks,
    part,
    r4,
    row_f,
    prob,
    r5,
    probf,
    num,
    r6,
    stat,
    r6s,
    hid,
    r7,
    hidf,
    load_sem,
    send_sem,
    recv_sem,
):
    d = lax.axis_index("dp")
    p = lax.axis_index("patch")
    z = d // 4
    x = d % 4
    q = x * 8 + p

    barrier = pltpu.get_barrier_semaphore()

    def greet_dp(k):
        pl.semaphore_signal(barrier, inc=1, device_id=((d + k) % DP, p), device_id_type=MESH)

    def plane_id(k):
        to = (q + k) % PLANE
        return to, (z * 4 + to // 8, to % 8)

    def greet_plane(k):
        to, device = plane_id(k)
        pl.semaphore_signal(barrier, inc=1, device_id=device, device_id_type=MESH)

    loop(DP, greet_dp)
    loop(PLANE, greet_plane)

    emb[992:1024, :] = jnp.zeros((32, 128), BF16)

    loads = []

    def load(src, dst):
        copy = pltpu.make_async_copy(src, dst, load_sem.at[len(loads)])
        copy.start()
        loads.append(copy)
        return copy

    l_emb = load(emb_ref.at[:, pl.ds(pl.multiple_of(p * 128, 128), 128)], emb.at[pl.ds(0, SLAB), :])
    l_q = load(wq_ref, wqkv.at[:, 0:128])
    l_k = load(wk_ref, wqkv.at[:, 128:256])
    l_v = load(wv_ref, wqkv.at[:, 256:384])
    l_pk = load(pk_ref, pk)
    l_pv = load(pv_ref, pv)
    l_wo = load(wo_ref, wo)
    l_cq = load(cq_ref, cq)
    l_ik = load(ik_ref, ik)
    l_iv = load(iv_ref, iv)
    l_co = load(co_ref, co)

    r256 = lax.broadcasted_iota(jnp.int32, (256, 128), 0)
    masks[...] = jnp.where(r256 // 16 == r256 % 16, 1.0, 0.0).astype(BF16)
    row_f[...] = jnp.zeros((64, 128), F32)

    l_emb.wait()
    lane1024 = lax.broadcasted_iota(jnp.int32, (128, 1024), 1)
    for c in range(4):
        col = jnp.broadcast_to(ids_ref[c : c + 1, :], (128, 128)).T - d * SLAB
        wide = jnp.concatenate([col] * 8, axis=1)
        onehot = jnp.where(wide == lane1024, 1.0, 0.0).astype(BF16)
        owned[c * 128 : (c + 1) * 128, :] = dot(onehot, emb[...]).astype(BF16)

    pl.semaphore_wait(barrier, (DP - 1) + (PLANE - 1))

    def await_bytes(ref, sem):
        pltpu.make_async_copy(ref, ref, sem).wait()

    def send1(k):
        to = (d + k) % DP
        pltpu.make_async_remote_copy(
            src_ref=owned.at[pl.ds(pl.multiple_of(to * 16, 16), 16), :],
            dst_ref=r1.at[d],
            send_sem=send_sem.at[0],
            recv_sem=recv_sem.at[0],
            device_id=(to, p),
            device_id_type=MESH,
        ).start()

    loop(DP, send1)
    r1[d] = owned[pl.ds(pl.multiple_of(d * 16, 16), 16), :]
    await_bytes(r1.at[pl.ds(0, DP - 1)], recv_sem.at[0])
    chunk = tree([r1[s] for s in range(DP)])
    tokc[...] = chunk
    r2[q] = chunk

    def send_plane(src_of, dst, n):
        def send(k):
            to, device = plane_id(k)
            pltpu.make_async_remote_copy(
                src_ref=src_of(to),
                dst_ref=dst.at[q],
                send_sem=send_sem.at[n],
                recv_sem=recv_sem.at[n],
                device_id=device,
                device_id_type=MESH,
            ).start()

        loop(PLANE, send)

    def await_plane(dst, n):
        await_bytes(dst.at[pl.ds(0, PLANE - 1)], recv_sem.at[n])

    send_plane(lambda to: tokc, r2, 1)
    l_q.wait()
    l_k.wait()
    l_v.wait()
    await_plane(r2, 1)

    toks = [
        jnp.concatenate([r2[b * 8 + j] for b in range(BEAMS)], axis=0).astype(F32)
        for j in range(CHUNKS)
    ]
    for j in range(CHUNKS):
        tokf[pl.ds(j, ROWS, stride=8), :] = toks[j]
    square = tree([t * t for t in toks])
    factor = lax.rsqrt(jnp.sum(square, axis=1, keepdims=True) * (1.0 / D) + 1e-06)
    sgain = sgain_ref[...].astype(F32)
    normed = jnp.concatenate(
        [(toks[j] * factor * sgain[j : j + 1, :]).astype(BF16) for j in range(CHUNKS)], axis=1
    )
    qkv = dot(normed, wqkv[...]).astype(BF16)
    tokf_q, tokf_k, tokf_v = (qkv[:, n * 128 : (n + 1) * 128].astype(F32) for n in range(3))
    queries = split_heads(tokf_q)
    own = jnp.sum(
        queries.astype(F32) * jnp.concatenate([tokf_k, tokf_k], axis=0), axis=1, keepdims=True
    )
    own = own * 0.125
    beam_row = pl.ds(pl.multiple_of(x * 16, 16), 16)
    num[0:ROWS, :] = tokf_k
    num[ROWS : 2 * ROWS, :] = tokf_v
    newk_ref[...] = num[beam_row, :].astype(BF16)
    newv_ref[...] = num[pl.ds(pl.multiple_of(ROWS + x * 16, 16), 16), :].astype(BF16)

    mask_of = [masks[i * 16 : (i + 1) * 16, :] for i in range(IMAGES)]

    def only(value, i):
        return (value.reshape(8, 16, 128) * mask_of[i][None]).reshape(128, 128)

    l_pk.wait()
    scores = tree(
        [dot_nt(only(queries, i), pk[i * LEN : (i + 1) * LEN, :]) for i in range(IMAGES)]
    )
    scores = scores * 0.125
    peak = jnp.maximum(jnp.max(scores, axis=1, keepdims=True), own)
    powers = jnp.exp(scores - peak)
    own_power = jnp.exp(own - peak)
    total = jnp.sum(powers, axis=1, keepdims=True) + own_power
    weights = powers.astype(BF16)
    own_weight = own_power.astype(BF16).astype(F32)
    l_pv.wait()
    context = tree(
        [dot(only(weights, i), pv[i * LEN : (i + 1) * LEN, :]) for i in range(IMAGES)]
    )
    context = (context + own_weight * jnp.concatenate([tokf_v, tokf_v], axis=0)) / total
    context = join_heads(context)
    pcol = jnp.broadcast_to(parents_ref[pl.ds(z // 2, 1), :], (128, 128)).T
    pcol = jnp.where(z % 2 == 0, pcol[:ROWS], pcol[ROWS:])
    context = jnp.where(pcol == x, context, 0.0).astype(BF16)

    l_wo.wait()
    projected = dot(context, wo[...])
    for j in range(CHUNKS):
        part[pl.ds(j, ROWS, stride=8), :] = projected[:, j * 128 : (j + 1) * 128]
    mine = pl.ds(pl.multiple_of(q * 16, 16), 16)

    def part_of(to):
        return part.at[pl.ds(pl.multiple_of(to * 16, 16), 16), :]

    send_plane(part_of, r4, 2)
    r4[q] = part[mine, :]
    l_cq.wait()
    await_plane(r4, 2)
    middle = tree([r4[s] for s in range(PLANE)]) + tokf[mine, :]

    cgain = cgain_ref[...].astype(F32)
    for r in range(2):
        row = middle[r * 8 : (r + 1) * 8, :]
        factor = lax.rsqrt(jnp.sum(row * row, keepdims=True) * (1.0 / D) + 1e-06)
        row_f[r * 8 : (r + 1) * 8, :] = row * factor * cgain

    def two_rows():
        return jnp.concatenate(
            [row_f[pl.ds(j, 8, stride=8), :] for j in range(CHUNKS)], axis=1
        ).astype(BF16)

    def back(value):
        for j in range(CHUNKS):
            row_f[pl.ds(j, 8, stride=8), :] = value[:, j * 128 : (j + 1) * 128]
        return row_f[0:16, :]

    mine_probe = back(dot(two_rows(), cq[...])).astype(BF16)
    prob[...] = mine_probe
    r5[q] = mine_probe

    send_plane(lambda to: prob, r5, 3)
    l_ik.wait()
    l_iv.wait()
    await_plane(r5, 3)
    probf[...] = r5[...].astype(F32).reshape(512, 128)

    same = lax.broadcasted_iota(jnp.int32, (128, 512), 0) % IMAGES == (
        lax.broadcasted_iota(jnp.int32, (128, 512), 1) // SPOTS
    )
    lane = lax.broadcasted_iota(jnp.int32, (ROWS, 128), 1)
    stats = jnp.zeros((ROWS, 128), F32)
    for j in range(CHUNKS):
        probes = split_heads(probf[pl.ds(j, ROWS, stride=8), :])
        block = slice(j * 128, (j + 1) * 128)
        scores = dot_nt(probes, ik[:, block]) * 0.125
        scores = jnp.where(same, scores, NEG)
        peak = jnp.max(scores, axis=1, keepdims=True)
        powers = jnp.exp(scores - peak)
        total = jnp.sum(powers, axis=1, keepdims=True)
        summed = join_heads(dot(powers.astype(BF16), iv[:, block]))
        num[pl.ds(j, ROWS, stride=8), :] = summed
        for h in range(2):
            rows = slice(h * ROWS, (h + 1) * ROWS)
            stats = jnp.where(lane == h * 8 + j, peak[rows], stats)
            stats = jnp.where(lane == 16 + h * 8 + j, total[rows], stats)
    stat[...] = stats

    def num_of(to):
        return num.at[pl.ds(pl.multiple_of(to * 16, 16), 16), :]

    def stat_of(to):
        return stat.at[pl.ds(pl.multiple_of(to * 2, 2), 2), :]

    send_plane(stat_of, r6s, 5)
    send_plane(num_of, r6, 4)
    r6[q] = num[mine, :]
    r6s[q] = stat[pl.ds(pl.multiple_of(q * 2, 2), 2), :]
    l_co.wait()
    await_plane(r6s, 5)
    stats = jnp.concatenate(
        [r6s[...].reshape(64, 128), jnp.zeros((64, 128), F32)], axis=0
    ).T
    lane8 = lax.broadcasted_iota(jnp.int32, (8, 128), 1)
    shares = []
    for r in range(2):
        valid = (lane8 < 64) & (lane8 % 2 == r)
        pair = []
        for h in range(2):
            peaks = jnp.where(valid, stats[h * 8 : (h + 1) * 8, :], NEG)
            totals = stats[16 + h * 8 : 16 + (h + 1) * 8, :]
            scale = jnp.where(valid, jnp.exp(peaks - jnp.max(peaks, axis=1, keepdims=True)), 0.0)
            pair.append((scale, jnp.sum(scale * totals, axis=1, keepdims=True)))
        shares.append(pair)
    await_plane(r6, 4)
    low = lane8 < 64
    for r in range(2):
        (scale0, total0), (scale1, total1) = shares[r]
        terms = []
        for s in range(PLANE):
            at = slice(2 * s + r, 2 * s + r + 1)
            scale = jnp.where(low, scale0[:, at], scale1[:, at])
            terms.append(r6[s, r * 8 : (r + 1) * 8, :] * scale)
        row_f[r * 8 : (r + 1) * 8, :] = tree(terms) / jnp.where(low, total0, total1)
    final = (back(dot(two_rows(), co[...])) + middle).astype(BF16)
    hid[...] = final
    r7[p] = final

    def send7(k):
        to = (p + k) % PATCH
        pltpu.make_async_remote_copy(
            src_ref=hid,
            dst_ref=r7.at[p],
            send_sem=send_sem.at[6],
            recv_sem=recv_sem.at[6],
            device_id=(d, to),
            device_id_type=MESH,
        ).start()

    loop(PATCH, send7)
    await_bytes(r7.at[pl.ds(0, PATCH - 1)], recv_sem.at[6])
    hidf[...] = r7[...].astype(F32).reshape(128, 128)
    for j in range(CHUNKS):
        hidden_ref[:, j * 128 : (j + 1) * 128] = hidf[pl.ds(j, 16, stride=8), :].astype(BF16)

    for n, ref in enumerate((r1, r2, r4, r5, r6, r6s)):
        await_bytes(ref.at[pl.ds(0, 31)], send_sem.at[n])
    await_bytes(r7.at[pl.ds(0, PATCH - 1)], send_sem.at[6])


def shards(
    token_ids,
    parents,
    embedding,
    self_gain,
    query_weight,
    key_weight,
    value_weight,
    output_weight,
    past_keys,
    past_values,
    cross_gain,
    cross_query,
    cross_output,
    image_keys,
    image_values,
):
    vmem = pl.BlockSpec(memory_space=pltpu.VMEM)
    hbm = pl.BlockSpec(memory_space=pl.ANY)
    return pl.pallas_call(
        kernel,
        out_shape=(
            jax.ShapeDtypeStruct((16, D), BF16),
            jax.ShapeDtypeStruct((16, 128), BF16),
            jax.ShapeDtypeStruct((16, 128), BF16),
        ),
        in_specs=[vmem, vmem, hbm, vmem, hbm, hbm, hbm, hbm, hbm, hbm, vmem, hbm, hbm, hbm, hbm],
        out_specs=(vmem, vmem, vmem),
        scratch_shapes=[
            pltpu.VMEM((1024, 128), BF16),
            pltpu.VMEM((D, 384), BF16),
            pltpu.VMEM((128, D), BF16),
            pltpu.VMEM((2048, 128), BF16),
            pltpu.VMEM((2048, 128), BF16),
            pltpu.VMEM((D, D), BF16),
            pltpu.VMEM((D, D), BF16),
            pltpu.VMEM((512, D), BF16),
            pltpu.VMEM((512, D), BF16),
            pltpu.VMEM((512, 128), BF16),
            pltpu.VMEM((DP, 16, 128), BF16),
            pltpu.VMEM((16, 128), BF16),
            pltpu.VMEM((PLANE, 16, 128), BF16),
            pltpu.VMEM((512, 128), F32),
            pltpu.VMEM((256, 128), BF16),
            pltpu.VMEM((512, 128), F32),
            pltpu.VMEM((PLANE, 16, 128), F32),
            pltpu.VMEM((64, 128), F32),
            pltpu.VMEM((16, 128), BF16),
            pltpu.VMEM((PLANE, 16, 128), BF16),
            pltpu.VMEM((512, 128), F32),
            pltpu.VMEM((512, 128), F32),
            pltpu.VMEM((PLANE, 16, 128), F32),
            pltpu.VMEM((ROWS, 128), F32),
            pltpu.VMEM((PLANE, 2, 128), F32),
            pltpu.VMEM((16, 128), BF16),
            pltpu.VMEM((PATCH, 16, 128), BF16),
            pltpu.VMEM((128, 128), F32),
            pltpu.SemaphoreType.DMA((11,)),
            pltpu.SemaphoreType.DMA((7,)),
            pltpu.SemaphoreType.DMA((7,)),
        ],
        compiler_params=pltpu.CompilerParams(collective_id=0, has_side_effects=True),
        name="step",
    )(
        token_ids.reshape(4, 128),
        parents.reshape(4, 128),
        embedding,
        self_gain.reshape(8, 128),
        query_weight,
        key_weight,
        value_weight,
        output_weight,
        past_keys.reshape(2048, 128),
        past_values.reshape(2048, 128),
        cross_gain.reshape(8, 128),
        cross_query,
        cross_output,
        image_keys.reshape(512, D),
        image_values.reshape(512, D),
    )


def solution(mesh):
    in_specs = (
        P(),
        P(),
        P("dp", None),
        P(),
        P(None, "patch"),
        P(None, "patch"),
        P(None, "patch"),
        P("patch", None),
        P("dp", None, "patch"),
        P("dp", None, "patch"),
        P(),
        P(),
        P(),
        P("dp", None, "patch", None),
        P("dp", None, "patch", None),
    )
    out_specs = (P("dp", None), P("dp", "patch"), P("dp", "patch"))
    return jax.shard_map(
        shards, mesh=mesh, in_specs=in_specs, out_specs=out_specs, check_vma=False
    )
```

```python
import jax
import jax.numpy as jnp
from jax import lax
from jax.experimental import pallas as pl
from jax.experimental.pallas import tpu as pltpu
from jax.sharding import PartitionSpec as P

MESH = pl.DeviceIdType.MESH
F32 = jnp.float32
BF16 = jnp.bfloat16

D = 1024
CHUNKS = 8
BEAMS = 4
IMAGES = 16
ROWS = BEAMS * IMAGES
DP = 32
PATCH = 8
PLANE = 32
SLAB = 1000
LEN = 128
SPOTS = 32
NEG = -1e30
NT = (((1,), (1,)), ((), ()))


def dot(a, b):
    return jnp.dot(a, b, preferred_element_type=F32)


def dot_nt(a, b):
    return lax.dot_general(a, b, NT, preferred_element_type=F32)


def tree(parts):
    while len(parts) > 1:
        parts = [a + b for a, b in zip(parts[::2], parts[1::2])] + (
            [parts[-1]] if len(parts) % 2 else []
        )
    return parts[0]


def hops(step, size):
    return min(step, size - step)


PARTNERS = sorted(
    [(dx, dy, dc) for dx in range(4) for dy in range(4) for dc in range(2) if dx + dy + dc],
    key=lambda t: -hops(t[0], 4) - hops(t[1], 4),
)
ACROSS = (2, 1, 3, 0)


def split_heads(x):
    lane = lax.broadcasted_iota(jnp.int32, x.shape, 1)
    low = jnp.where(lane < 64, x, 0.0)
    high = jnp.where(lane < 64, 0.0, x)
    return jnp.concatenate([low, high], axis=0).astype(BF16)


def join_heads(x):
    half = x.shape[0] // 2
    lane = lax.broadcasted_iota(jnp.int32, (half, 128), 1)
    return jnp.where(lane < 64, x[:half], x[half:])


def kernel(
    ids_hbm,
    parents_hbm,
    emb_ref,
    sgain_hbm,
    wq_ref,
    wk_ref,
    wv_ref,
    wo_ref,
    pk_ref,
    pv_ref,
    cgain_hbm,
    cq_ref,
    co_ref,
    ik_ref,
    iv_ref,
    hidden_ref,
    newk_ref,
    newv_ref,
    ids_ref,
    parents_ref,
    sgain_ref,
    cgain_ref,
    emb,
    wqkv,
    wo,
    pk,
    pv,
    cq,
    co,
    ik,
    iv,
    onehot,
    owned,
    r1,
    tokc,
    r2,
    tokf,
    masks,
    part,
    partb,
    r4,
    row_f,
    prob,
    r5,
    probf,
    num,
    numb,
    r6,
    stat,
    r6s,
    hid,
    r7,
    hidf,
    load_sem,
    send_sem,
    recv_sem,
    ready,
):
    d = lax.axis_index("dp")
    p = lax.axis_index("patch")
    z, x = d // 4, d % 4
    y, c = p // 2, p % 2
    q = x * 8 + p
    zs = [lax.rem(z + k, 8) for k in range(8)]
    xs = [lax.rem(x + k, 4) for k in range(4)]
    ys = [lax.rem(y + k, 4) for k in range(4)]
    cs = [c, 1 - c]

    loads = []

    def load(src, dst):
        copy = pltpu.make_async_copy(src, dst, load_sem.at[len(loads)])
        copy.start()
        loads.append(copy)
        return copy

    emb[992:1024, :] = jnp.zeros((32, 128), BF16)
    l_ids = load(ids_hbm, ids_ref)
    l_emb = load(emb_ref.at[:, pl.ds(pl.multiple_of(p * 128, 128), 128)], emb.at[pl.ds(0, SLAB), :])

    barrier = pltpu.get_barrier_semaphore()

    def signal(sem, device):
        pl.semaphore_signal(sem, inc=1, device_id=device, device_id_type=MESH)

    for dz in range(1, 8):

        @pl.when(z + dz < 8)
        def _(dz=dz):
            for dx in ACROSS:
                signal(barrier, (zs[dz] * 4 + xs[dx], p))

    for dx, dy, dc in PARTNERS:
        signal(barrier, (z * 4 + xs[dx], ys[dy] * 2 + cs[dc]))

    l_q = load(wq_ref, wqkv.at[:, 0:128])
    l_k = load(wk_ref, wqkv.at[:, 128:256])
    l_v = load(wv_ref, wqkv.at[:, 256:384])
    l_gain = load(sgain_hbm, sgain_ref)
    l_parents = load(parents_hbm, parents_ref)
    l_pk = load(pk_ref, pk)
    l_pv = load(pv_ref, pv)
    l_wo = load(wo_ref, wo)
    l_cgain = load(cgain_hbm, cgain_ref)
    l_cq = load(cq_ref, cq)
    l_ik = load(ik_ref, ik)
    l_iv = load(iv_ref, iv)
    l_co = load(co_ref, co)

    r256 = lax.broadcasted_iota(jnp.int32, (256, 128), 0)
    masks[...] = jnp.where(r256 // 16 == r256 % 16, 1.0, 0.0).astype(BF16)
    row_f[...] = jnp.zeros((64, 128), F32)

    l_ids.wait()
    lane1024 = lax.broadcasted_iota(jnp.int32, (128, 1024), 1)
    for n in range(4):
        col = jnp.broadcast_to(ids_ref[n : n + 1, :], (128, 128)).T - d * SLAB
        wide = jnp.concatenate([col] * 8, axis=1)
        onehot[n * 128 : (n + 1) * 128, :] = jnp.where(wide == lane1024, 1.0, 0.0).astype(BF16)
    l_emb.wait()
    for n in range(4):
        rows = slice(n * 128, (n + 1) * 128)
        owned[rows, :] = dot(onehot[rows, :], emb[...]).astype(BF16)

    pl.semaphore_wait(barrier, (PLANE - 1) + 4 * z)
    for dz in range(1, 8):

        @pl.when(z + dz >= 8)
        def _(dz=dz):
            for dx in ACROSS:
                signal(ready.at[z], (zs[dz] * 4 + xs[dx], p))

    def await_bytes(ref, sem):
        pltpu.make_async_copy(ref, ref, sem).wait()

    def send1(dz, dx):
        to = zs[dz] * 4 + xs[dx]
        pltpu.make_async_remote_copy(
            src_ref=owned.at[pl.ds(pl.multiple_of(to * 16, 16), 16), :],
            dst_ref=r1.at[d],
            send_sem=send_sem.at[0],
            recv_sem=recv_sem.at[0],
            device_id=(to, p),
            device_id_type=MESH,
        ).start()

    for dz in (4, 3, 5, 2, 6, 1, 7):

        @pl.when(z + dz >= 8)
        def _(dz=dz):
            for dx in ACROSS:
                send1(dz, dx)

    for dx in ACROSS[:3]:
        send1(0, dx)
    for dz in range(1, 8):

        @pl.when(z + dz < 8)
        def _(dz=dz):
            pl.semaphore_wait(ready.at[zs[dz]], 4)
            for dx in ACROSS:
                send1(dz, dx)

    r1[d] = owned[pl.ds(pl.multiple_of(d * 16, 16), 16), :]
    await_bytes(r1.at[pl.ds(0, DP - 1)], recv_sem.at[0])
    chunk = tree([r1[s] for s in range(DP)])
    tokc[...] = chunk
    r2[q] = chunk

    def send_plane(src_of, dst, n, partners=PARTNERS):
        for dx, dy, dc in partners:
            to_x, to_p = xs[dx], ys[dy] * 2 + cs[dc]
            pltpu.make_async_remote_copy(
                src_ref=src_of(to_x, to_p),
                dst_ref=dst,
                send_sem=send_sem.at[n],
                recv_sem=recv_sem.at[n],
                device_id=(z * 4 + to_x, to_p),
                device_id_type=MESH,
            ).start()

    def await_plane(dst, n):
        await_bytes(dst.at[pl.ds(0, PLANE - 1)], recv_sem.at[n])

    send_plane(lambda to_x, to_p: tokc, r2.at[q], 1)
    l_q.wait()
    l_k.wait()
    l_v.wait()
    l_gain.wait()
    await_plane(r2, 1)

    toks = [
        jnp.concatenate([r2[b * 8 + j] for b in range(BEAMS)], axis=0).astype(F32)
        for j in range(CHUNKS)
    ]
    for j in range(CHUNKS):
        tokf[pl.ds(j, ROWS, stride=8), :] = toks[j]
    square = tree([t * t for t in toks])
    factor = lax.rsqrt(jnp.sum(square, axis=1, keepdims=True) * (1.0 / D) + 1e-06)
    sgain = sgain_ref[...].astype(F32)
    normed = jnp.concatenate(
        [(toks[j] * factor * sgain[j : j + 1, :]).astype(BF16) for j in range(CHUNKS)], axis=1
    )
    qkv = dot(normed, wqkv[...]).astype(BF16)
    new_q, new_k, new_v = (qkv[:, n * 128 : (n + 1) * 128].astype(F32) for n in range(3))
    queries = split_heads(new_q)
    own = jnp.sum(
        queries.astype(F32) * jnp.concatenate([new_k, new_k], axis=0), axis=1, keepdims=True
    )
    own = own * 0.125
    hidf[0:ROWS, :] = new_k
    hidf[ROWS : 2 * ROWS, :] = new_v
    newk_ref[...] = hidf[pl.ds(pl.multiple_of(x * 16, 16), 16), :].astype(BF16)
    newv_ref[...] = hidf[pl.ds(pl.multiple_of(ROWS + x * 16, 16), 16), :].astype(BF16)

    mask_of = [masks[i * 16 : (i + 1) * 16, :] for i in range(IMAGES)]

    def only(value, i):
        return (value.reshape(8, 16, 128) * mask_of[i][None]).reshape(128, 128)

    l_pk.wait()
    scores = tree(
        [dot_nt(only(queries, i), pk[i * LEN : (i + 1) * LEN, :]) for i in range(IMAGES)]
    )
    scores = scores * 0.125
    peak = jnp.maximum(jnp.max(scores, axis=1, keepdims=True), own)
    powers = jnp.exp(scores - peak)
    own_power = jnp.exp(own - peak)
    total = jnp.sum(powers, axis=1, keepdims=True) + own_power
    weights = powers.astype(BF16)
    own_weight = own_power.astype(BF16).astype(F32)
    l_pv.wait()
    context = tree(
        [dot(only(weights, i), pv[i * LEN : (i + 1) * LEN, :]) for i in range(IMAGES)]
    )
    context = (context + own_weight * jnp.concatenate([new_v, new_v], axis=0)) / total
    context = join_heads(context)
    l_parents.wait()
    pcol = jnp.broadcast_to(parents_ref[pl.ds(z // 2, 1), :], (128, 128)).T
    pcol = jnp.where(z % 2 == 0, pcol[:ROWS], pcol[ROWS:])
    context = jnp.where(pcol == x, context, 0.0).astype(BF16)

    l_wo.wait()
    projected = dot(context, wo[...])
    for j in range(CHUNKS):
        part[pl.ds(j, ROWS, stride=8), :] = projected[:, j * 128 : (j + 1) * 128]
    partb[...] = part[...].astype(BF16)
    mine = pl.ds(pl.multiple_of(q * 16, 16), 16)

    def part_of(to_x, to_p):
        return partb.at[pl.ds(pl.multiple_of((to_x * 8 + to_p) * 16, 16), 16), :]

    send_plane(part_of, r4.at[q], 2)
    r4[q] = partb[mine, :]
    l_cgain.wait()
    l_cq.wait()
    await_plane(r4, 2)
    middle = tree([r4[s].astype(F32) for s in range(PLANE)]) + tokf[mine, :]

    cgain = cgain_ref[...].astype(F32)
    for r in range(2):
        row = middle[r * 8 : (r + 1) * 8, :]
        factor = lax.rsqrt(jnp.sum(row * row, keepdims=True) * (1.0 / D) + 1e-06)
        row_f[r * 8 : (r + 1) * 8, :] = row * factor * cgain

    def two_rows():
        return jnp.concatenate(
            [row_f[pl.ds(j, 8, stride=8), :] for j in range(CHUNKS)], axis=1
        ).astype(BF16)

    def back(value):
        for j in range(CHUNKS):
            row_f[pl.ds(j, 8, stride=8), :] = value[:, j * 128 : (j + 1) * 128]
        return row_f[0:16, :]

    mine_probe = back(dot(two_rows(), cq[...])).astype(BF16)
    prob[...] = mine_probe
    slot = p * 4 + x
    r5[slot] = mine_probe

    send_plane(lambda to_x, to_p: prob, r5.at[slot], 3)
    l_ik.wait()
    l_iv.wait()
    await_plane(r5, 3)

    row32 = lax.broadcasted_iota(jnp.int32, (32, 128), 0)
    image = (row32 // 8 % 2) * 2 + row32 % 2
    same = image == lax.broadcasted_iota(jnp.int32, (32, 128), 1) // SPOTS
    lane = lax.broadcasted_iota(jnp.int32, (16, 128), 1)
    for g, dy in enumerate(ACROSS):
        base = pl.multiple_of(ys[dy] * 128, 128)
        here = slice(g * 128, (g + 1) * 128)
        probf[here, :] = r5[pl.ds(ys[dy] * 8, 8)].astype(F32).reshape(128, 128)
        stats = jnp.zeros((16, 128), F32)
        for j in range(CHUNKS):
            block = slice(j * 128, (j + 1) * 128)
            probes = split_heads(probf[pl.ds(g * 128 + j, 16, stride=8), :])
            scores = dot_nt(probes, ik[pl.ds(base, 128), block]) * 0.125
            scores = jnp.where(same, scores, NEG)
            peak = jnp.max(scores, axis=1, keepdims=True)
            powers = jnp.exp(scores - peak)
            total = jnp.sum(powers, axis=1, keepdims=True)
            summed = join_heads(dot(powers.astype(BF16), iv[pl.ds(base, 128), block]))
            num[pl.ds(g * 128 + j, 16, stride=8), :] = summed
            for h in range(2):
                rows = slice(h * 16, (h + 1) * 16)
                stats = jnp.where(lane == h * 8 + j, peak[rows], stats)
                stats = jnp.where(lane == 16 + h * 8 + j, total[rows], stats)
        stat[g * 16 : (g + 1) * 16, :] = stats
        numb[here, :] = num[here, :].astype(BF16)

        def num_of(to_x, to_p, g=g):
            at = g * 128 + ((to_p % 2) * 4 + to_x) * 16
            return numb.at[pl.ds(pl.multiple_of(at, 16), 16), :]

        def stat_of(to_x, to_p, g=g):
            at = g * 16 + ((to_p % 2) * 4 + to_x) * 2
            return stat.at[pl.ds(pl.multiple_of(at, 2), 2), :]

        group = [t for t in PARTNERS if t[1] == dy]
        send_plane(stat_of, r6s.at[q], 5, group)
        send_plane(num_of, r6.at[q], 4, group)
    own_at = 3 * 128 + (c * 4 + x) * 16
    r6[q] = numb[pl.ds(pl.multiple_of(own_at, 16), 16), :]
    r6s[q] = stat[pl.ds(pl.multiple_of(48 + (c * 4 + x) * 2, 2), 2), :]
    l_co.wait()
    await_plane(r6s, 5)
    stats = jnp.concatenate(
        [r6s[...].reshape(64, 128), jnp.zeros((64, 128), F32)], axis=0
    ).T
    lane8 = lax.broadcasted_iota(jnp.int32, (8, 128), 1)
    shares = []
    for r in range(2):
        valid = (lane8 < 64) & (lane8 % 2 == r)
        pair = []
        for h in range(2):
            peaks = jnp.where(valid, stats[h * 8 : (h + 1) * 8, :], NEG)
            totals = stats[16 + h * 8 : 16 + (h + 1) * 8, :]
            scale = jnp.where(valid, jnp.exp(peaks - jnp.max(peaks, axis=1, keepdims=True)), 0.0)
            pair.append((scale, jnp.sum(scale * totals, axis=1, keepdims=True)))
        shares.append(pair)
    await_plane(r6, 4)
    low = lane8 < 64
    for r in range(2):
        (scale0, total0), (scale1, total1) = shares[r]
        terms = []
        for s in range(PLANE):
            at = slice(2 * s + r, 2 * s + r + 1)
            scale = jnp.where(low, scale0[:, at], scale1[:, at])
            terms.append(r6[s].astype(F32)[r * 8 : (r + 1) * 8, :] * scale)
        row_f[r * 8 : (r + 1) * 8, :] = tree(terms) / jnp.where(low, total0, total1)
    final = (back(dot(two_rows(), co[...])) + middle).astype(BF16)
    hid[...] = final
    r7[p] = final

    for dx, dy, dc in PARTNERS:
        if dx == 0:
            pltpu.make_async_remote_copy(
                src_ref=hid,
                dst_ref=r7.at[p],
                send_sem=send_sem.at[6],
                recv_sem=recv_sem.at[6],
                device_id=(d, ys[dy] * 2 + cs[dc]),
                device_id_type=MESH,
            ).start()
    for n, ref in enumerate((r1, r2, r4, r5, r6, r6s)):
        await_bytes(ref.at[pl.ds(0, 31)], send_sem.at[n])
    await_bytes(r7.at[pl.ds(0, PATCH - 1)], recv_sem.at[6])
    hidf[...] = r7[...].astype(F32).reshape(128, 128)
    for j in range(CHUNKS):
        hidden_ref[:, j * 128 : (j + 1) * 128] = hidf[pl.ds(j, 16, stride=8), :].astype(BF16)
    await_bytes(r7.at[pl.ds(0, PATCH - 1)], send_sem.at[6])


def emit(hidden, new_k, new_v, hidden_ref, newk_ref, newv_ref):
    hidden_ref[...] = hidden[...]
    newk_ref[...] = new_k[...]
    newv_ref[...] = new_v[...]


def shards(
    token_ids,
    parents,
    embedding,
    self_gain,
    query_weight,
    key_weight,
    value_weight,
    output_weight,
    past_keys,
    past_values,
    cross_gain,
    cross_query,
    cross_output,
    image_keys,
    image_values,
):
    vmem = pl.BlockSpec(memory_space=pltpu.VMEM)
    hbm = pl.BlockSpec(memory_space=pl.ANY)
    shapes = ((16, D), (16, 128), (16, 128))
    results = pl.pallas_call(
        kernel,
        out_shape=tuple(pltpu.VMEM(shape, BF16) for shape in shapes),
        in_specs=[hbm] * 15,
        out_specs=(vmem, vmem, vmem),
        scratch_shapes=[
            pltpu.VMEM((4, 128), jnp.int32),
            pltpu.VMEM((4, 128), jnp.int32),
            pltpu.VMEM((8, 128), BF16),
            pltpu.VMEM((8, 128), BF16),
            pltpu.VMEM((1024, 128), BF16),
            pltpu.VMEM((D, 384), BF16),
            pltpu.VMEM((128, D), BF16),
            pltpu.VMEM((2048, 128), BF16),
            pltpu.VMEM((2048, 128), BF16),
            pltpu.VMEM((D, D), BF16),
            pltpu.VMEM((D, D), BF16),
            pltpu.VMEM((512, D), BF16),
            pltpu.VMEM((512, D), BF16),
            pltpu.VMEM((512, D), BF16),
            pltpu.VMEM((512, 128), BF16),
            pltpu.VMEM((DP, 16, 128), BF16),
            pltpu.VMEM((16, 128), BF16),
            pltpu.VMEM((PLANE, 16, 128), BF16),
            pltpu.VMEM((512, 128), F32),
            pltpu.VMEM((256, 128), BF16),
            pltpu.VMEM((512, 128), F32),
            pltpu.VMEM((512, 128), BF16),
            pltpu.VMEM((PLANE, 16, 128), BF16),
            pltpu.VMEM((64, 128), F32),
            pltpu.VMEM((16, 128), BF16),
            pltpu.VMEM((PLANE, 16, 128), BF16),
            pltpu.VMEM((512, 128), F32),
            pltpu.VMEM((512, 128), F32),
            pltpu.VMEM((512, 128), BF16),
            pltpu.VMEM((PLANE, 16, 128), BF16),
            pltpu.VMEM((ROWS, 128), F32),
            pltpu.VMEM((PLANE, 2, 128), F32),
            pltpu.VMEM((16, 128), BF16),
            pltpu.VMEM((PATCH, 16, 128), BF16),
            pltpu.VMEM((128, 128), F32),
            pltpu.SemaphoreType.DMA((15,)),
            pltpu.SemaphoreType.DMA((7,)),
            pltpu.SemaphoreType.DMA((7,)),
            pltpu.SemaphoreType.REGULAR((8,)),
        ],
        compiler_params=pltpu.CompilerParams(collective_id=0, has_side_effects=True),
        name="step",
    )(
        token_ids.reshape(4, 128),
        parents.reshape(4, 128),
        embedding,
        self_gain.reshape(8, 128),
        query_weight,
        key_weight,
        value_weight,
        output_weight,
        past_keys.reshape(2048, 128),
        past_values.reshape(2048, 128),
        cross_gain.reshape(8, 128),
        cross_query,
        cross_output,
        image_keys.reshape(512, D),
        image_values.reshape(512, D),
    )
    return pl.pallas_call(
        emit,
        out_shape=tuple(jax.ShapeDtypeStruct(shape, BF16) for shape in shapes),
        in_specs=[vmem] * 3,
        out_specs=(vmem, vmem, vmem),
        name="emit",
    )(*[pltpu.with_memory_space_constraint(r, pltpu.VMEM) for r in results])


def solution(mesh):
    in_specs = (
        P(),
        P(),
        P("dp", None),
        P(),
        P(None, "patch"),
        P(None, "patch"),
        P(None, "patch"),
        P("patch", None),
        P("dp", None, "patch"),
        P("dp", None, "patch"),
        P(),
        P(),
        P(),
        P("dp", None, "patch", None),
        P("dp", None, "patch", None),
    )
    out_specs = (P("dp", None), P("dp", "patch"), P("dp", "patch"))
    return jax.shard_map(
        shards, mesh=mesh, in_specs=in_specs, out_specs=out_specs, check_vma=False
    )
```

```python
import jax
import jax.numpy as jnp
from jax import lax
from jax.experimental import pallas as pl
from jax.experimental.pallas import tpu as pltpu
from jax.sharding import PartitionSpec as P

MESH = pl.DeviceIdType.MESH
F32 = jnp.float32
BF16 = jnp.bfloat16

D = 1024
CHUNKS = 8
BEAMS = 4
IMAGES = 16
ROWS = BEAMS * IMAGES
DP = 32
PATCH = 8
PLANE = 32
SLAB = 1000
LEN = 128
SPOTS = 32
NEG = -1e30
NT = (((1,), (1,)), ((), ()))


def dot(a, b):
    return jnp.dot(a, b, preferred_element_type=F32)


def dot_nt(a, b):
    return lax.dot_general(a, b, NT, preferred_element_type=F32)


def tree(parts):
    while len(parts) > 1:
        parts = [a + b for a, b in zip(parts[::2], parts[1::2])] + (
            [parts[-1]] if len(parts) % 2 else []
        )
    return parts[0]


def hops(step, size):
    return min(step, size - step)


PARTNERS = sorted(
    [(dx, dy, dc) for dx in range(4) for dy in range(4) for dc in range(2) if dx + dy + dc],
    key=lambda t: -hops(t[0], 4) - hops(t[1], 4),
)
ACROSS = (2, 1, 3, 0)


def split_heads(x):
    lane = lax.broadcasted_iota(jnp.int32, x.shape, 1)
    low = jnp.where(lane < 64, x, 0.0)
    high = jnp.where(lane < 64, 0.0, x)
    return jnp.concatenate([low, high], axis=0).astype(BF16)


def join_heads(x):
    half = x.shape[0] // 2
    lane = lax.broadcasted_iota(jnp.int32, (half, 128), 1)
    return jnp.where(lane < 64, x[:half], x[half:])


def kernel(
    ids_hbm,
    parents_hbm,
    emb_ref,
    sgain_hbm,
    wq_ref,
    wk_ref,
    wv_ref,
    wo_ref,
    pk_ref,
    pv_ref,
    cgain_hbm,
    cq_ref,
    co_ref,
    ik_ref,
    iv_ref,
    hidden_ref,
    newk_ref,
    newv_ref,
    ids_ref,
    parents_ref,
    sgain_ref,
    cgain_ref,
    emb,
    wqkv,
    wo,
    pk,
    pv,
    cq,
    co,
    ik,
    iv,
    onehot,
    owned,
    r1,
    tokc,
    r2,
    tokf,
    masks,
    part,
    partb,
    r4,
    row_f,
    prob,
    r5,
    probf,
    num,
    numb,
    r6,
    stat,
    r6s,
    hid,
    r7,
    hidf,
    load_sem,
    send_sem,
    recv_sem,
    ready,
    in_plane,
):
    d = lax.axis_index("dp")
    p = lax.axis_index("patch")
    z, x = d // 4, d % 4
    y, c = p // 2, p % 2
    q = x * 8 + p
    zs = [lax.rem(z + k, 8) for k in range(8)]
    xs = [lax.rem(x + k, 4) for k in range(4)]
    ys = [lax.rem(y + k, 4) for k in range(4)]
    cs = [c, 1 - c]

    loads = []

    def load(src, dst):
        copy = pltpu.make_async_copy(src, dst, load_sem.at[len(loads)])
        copy.start()
        loads.append(copy)
        return copy

    emb[992:1024, :] = jnp.zeros((32, 128), BF16)
    l_ids = load(ids_hbm, ids_ref)
    l_emb = load(emb_ref.at[:, pl.ds(pl.multiple_of(p * 128, 128), 128)], emb.at[pl.ds(0, SLAB), :])

    barrier = pltpu.get_barrier_semaphore()

    def signal(sem, device):
        pl.semaphore_signal(sem, inc=1, device_id=device, device_id_type=MESH)

    ps = [lax.rem(p + k, 8) for k in range(8)]

    def later(of_z, of_plane):
        for dz in range(1, 8):

            @pl.when(z + dz < 8)
            def _(dz=dz):
                for dx in ACROSS:
                    signal(of_z, (zs[dz] * 4 + xs[dx], p))

        for dx in range(1, 4):

            @pl.when(x + dx < 4)
            def _(dx=dx):
                for k in range(8):
                    signal(of_plane, (z * 4 + xs[dx], ps[k]))

        for k in range(1, 8):

            @pl.when(p + k < 8)
            def _(k=k):
                signal(of_plane, (d, ps[k]))

    def earlier(of_z, of_plane):
        for dz in range(1, 8):

            @pl.when(z + dz >= 8)
            def _(dz=dz):
                for dx in ACROSS:
                    signal(of_z, (zs[dz] * 4 + xs[dx], p))

        for dx in range(1, 4):

            @pl.when(x + dx >= 4)
            def _(dx=dx):
                for k in range(8):
                    signal(of_plane, (z * 4 + xs[dx], ps[k]))

        for k in range(1, 8):

            @pl.when(p + k >= 8)
            def _(k=k):
                signal(of_plane, (d, ps[k]))

    later(barrier, barrier)

    l_q = load(wq_ref, wqkv.at[:, 0:128])
    l_k = load(wk_ref, wqkv.at[:, 128:256])
    l_v = load(wv_ref, wqkv.at[:, 256:384])
    l_gain = load(sgain_hbm, sgain_ref)
    l_parents = load(parents_hbm, parents_ref)
    l_pk = load(pk_ref, pk)
    l_pv = load(pv_ref, pv)
    l_wo = load(wo_ref, wo)
    l_cgain = load(cgain_hbm, cgain_ref)
    l_cq = load(cq_ref, cq)
    l_ik = load(ik_ref, ik)
    l_iv = load(iv_ref, iv)
    l_co = load(co_ref, co)

    @pl.when(4 * z + q > 0)
    def _():
        pl.semaphore_wait(barrier, 4 * z + q)

    earlier(ready.at[z], in_plane)

    r256 = lax.broadcasted_iota(jnp.int32, (256, 128), 0)
    masks[...] = jnp.where(r256 // 16 == r256 % 16, 1.0, 0.0).astype(BF16)
    row_f[...] = jnp.zeros((64, 128), F32)

    l_ids.wait()
    lane1024 = lax.broadcasted_iota(jnp.int32, (128, 1024), 1)
    for n in range(4):
        col = jnp.broadcast_to(ids_ref[n : n + 1, :], (128, 128)).T - d * SLAB
        wide = jnp.concatenate([col] * 8, axis=1)
        onehot[n * 128 : (n + 1) * 128, :] = jnp.where(wide == lane1024, 1.0, 0.0).astype(BF16)
    l_emb.wait()
    for n in range(4):
        rows = slice(n * 128, (n + 1) * 128)
        owned[rows, :] = dot(onehot[rows, :], emb[...]).astype(BF16)

    def await_bytes(ref, sem):
        pltpu.make_async_copy(ref, ref, sem).wait()

    def send1(dz, dx):
        to = zs[dz] * 4 + xs[dx]
        pltpu.make_async_remote_copy(
            src_ref=owned.at[pl.ds(pl.multiple_of(to * 16, 16), 16), :],
            dst_ref=r1.at[d],
            send_sem=send_sem.at[0],
            recv_sem=recv_sem.at[0],
            device_id=(to, p),
            device_id_type=MESH,
        ).start()

    for dz in (4, 3, 5, 2, 6, 1, 7):

        @pl.when(z + dz >= 8)
        def _(dz=dz):
            for dx in ACROSS:
                send1(dz, dx)


    @pl.when(q < PLANE - 1)
    def _():
        pl.semaphore_wait(in_plane, (PLANE - 1) - q)

    for dx in ACROSS[:3]:
        send1(0, dx)
    for dz in range(1, 8):

        @pl.when(z + dz < 8)
        def _(dz=dz):
            pl.semaphore_wait(ready.at[zs[dz]], 4)
            for dx in ACROSS:
                send1(dz, dx)

    r1[d] = owned[pl.ds(pl.multiple_of(d * 16, 16), 16), :]
    await_bytes(r1.at[pl.ds(0, DP - 1)], recv_sem.at[0])
    chunk = tree([r1[s] for s in range(DP)])
    tokc[...] = chunk
    r2[q] = chunk

    def send_plane(src_of, dst, n, partners=PARTNERS):
        for dx, dy, dc in partners:
            to_x, to_p = xs[dx], ys[dy] * 2 + cs[dc]
            pltpu.make_async_remote_copy(
                src_ref=src_of(to_x, to_p),
                dst_ref=dst,
                send_sem=send_sem.at[n],
                recv_sem=recv_sem.at[n],
                device_id=(z * 4 + to_x, to_p),
                device_id_type=MESH,
            ).start()

    def await_plane(dst, n):
        await_bytes(dst.at[pl.ds(0, PLANE - 1)], recv_sem.at[n])

    send_plane(lambda to_x, to_p: tokc, r2.at[q], 1)
    l_q.wait()
    l_k.wait()
    l_v.wait()
    l_gain.wait()
    await_plane(r2, 1)

    toks = [
        jnp.concatenate([r2[b * 8 + j] for b in range(BEAMS)], axis=0).astype(F32)
        for j in range(CHUNKS)
    ]
    for j in range(CHUNKS):
        tokf[pl.ds(j, ROWS, stride=8), :] = toks[j]
    square = tree([t * t for t in toks])
    factor = lax.rsqrt(jnp.sum(square, axis=1, keepdims=True) * (1.0 / D) + 1e-06)
    sgain = sgain_ref[...].astype(F32)
    normed = jnp.concatenate(
        [(toks[j] * factor * sgain[j : j + 1, :]).astype(BF16) for j in range(CHUNKS)], axis=1
    )
    qkv = dot(normed, wqkv[...]).astype(BF16)
    new_q, new_k, new_v = (qkv[:, n * 128 : (n + 1) * 128].astype(F32) for n in range(3))
    queries = split_heads(new_q)
    own = jnp.sum(
        queries.astype(F32) * jnp.concatenate([new_k, new_k], axis=0), axis=1, keepdims=True
    )
    own = own * 0.125
    hidf[0:ROWS, :] = new_k
    hidf[ROWS : 2 * ROWS, :] = new_v
    newk_ref[...] = hidf[pl.ds(pl.multiple_of(x * 16, 16), 16), :].astype(BF16)
    newv_ref[...] = hidf[pl.ds(pl.multiple_of(ROWS + x * 16, 16), 16), :].astype(BF16)

    mask_of = [masks[i * 16 : (i + 1) * 16, :] for i in range(IMAGES)]

    def only(value, i):
        return (value.reshape(8, 16, 128) * mask_of[i][None]).reshape(128, 128)

    l_pk.wait()
    scores = tree(
        [dot_nt(only(queries, i), pk[i * LEN : (i + 1) * LEN, :]) for i in range(IMAGES)]
    )
    scores = scores * 0.125
    peak = jnp.maximum(jnp.max(scores, axis=1, keepdims=True), own)
    powers = jnp.exp(scores - peak)
    own_power = jnp.exp(own - peak)
    total = jnp.sum(powers, axis=1, keepdims=True) + own_power
    weights = powers.astype(BF16)
    own_weight = own_power.astype(BF16).astype(F32)
    l_pv.wait()
    context = tree(
        [dot(only(weights, i), pv[i * LEN : (i + 1) * LEN, :]) for i in range(IMAGES)]
    )
    context = (context + own_weight * jnp.concatenate([new_v, new_v], axis=0)) / total
    context = join_heads(context)
    l_parents.wait()
    pcol = jnp.broadcast_to(parents_ref[pl.ds(z // 2, 1), :], (128, 128)).T
    pcol = jnp.where(z % 2 == 0, pcol[:ROWS], pcol[ROWS:])
    context = jnp.where(pcol == x, context, 0.0).astype(BF16)

    l_wo.wait()
    projected = dot(context, wo[...])
    for j in range(CHUNKS):
        part[pl.ds(j, ROWS, stride=8), :] = projected[:, j * 128 : (j + 1) * 128]
    partb[...] = part[...].astype(BF16)
    mine = pl.ds(pl.multiple_of(q * 16, 16), 16)

    def part_of(to_x, to_p):
        return partb.at[pl.ds(pl.multiple_of((to_x * 8 + to_p) * 16, 16), 16), :]

    send_plane(part_of, r4.at[q], 2)
    r4[q] = partb[mine, :]
    l_cgain.wait()
    l_cq.wait()
    await_plane(r4, 2)
    middle = tree([r4[s].astype(F32) for s in range(PLANE)]) + tokf[mine, :]

    cgain = cgain_ref[...].astype(F32)
    for r in range(2):
        row = middle[r * 8 : (r + 1) * 8, :]
        factor = lax.rsqrt(jnp.sum(row * row, keepdims=True) * (1.0 / D) + 1e-06)
        row_f[r * 8 : (r + 1) * 8, :] = row * factor * cgain

    def two_rows():
        return jnp.concatenate(
            [row_f[pl.ds(j, 8, stride=8), :] for j in range(CHUNKS)], axis=1
        ).astype(BF16)

    def back(value):
        for j in range(CHUNKS):
            row_f[pl.ds(j, 8, stride=8), :] = value[:, j * 128 : (j + 1) * 128]
        return row_f[0:16, :]

    mine_probe = back(dot(two_rows(), cq[...])).astype(BF16)
    prob[...] = mine_probe
    slot = p * 4 + x
    r5[slot] = mine_probe

    send_plane(lambda to_x, to_p: prob, r5.at[slot], 3)
    l_ik.wait()
    l_iv.wait()
    await_plane(r5, 3)

    row32 = lax.broadcasted_iota(jnp.int32, (32, 128), 0)
    image = (row32 // 8 % 2) * 2 + row32 % 2
    same = image == lax.broadcasted_iota(jnp.int32, (32, 128), 1) // SPOTS
    lane = lax.broadcasted_iota(jnp.int32, (16, 128), 1)
    for g, dy in enumerate(ACROSS):
        base = pl.multiple_of(ys[dy] * 128, 128)
        here = slice(g * 128, (g + 1) * 128)
        probf[here, :] = r5[pl.ds(ys[dy] * 8, 8)].astype(F32).reshape(128, 128)
        stats = jnp.zeros((16, 128), F32)
        for j in range(CHUNKS):
            block = slice(j * 128, (j + 1) * 128)
            probes = split_heads(probf[pl.ds(g * 128 + j, 16, stride=8), :])
            scores = dot_nt(probes, ik[pl.ds(base, 128), block]) * 0.125
            scores = jnp.where(same, scores, NEG)
            peak = jnp.max(scores, axis=1, keepdims=True)
            powers = jnp.exp(scores - peak)
            total = jnp.sum(powers, axis=1, keepdims=True)
            summed = join_heads(dot(powers.astype(BF16), iv[pl.ds(base, 128), block]))
            num[pl.ds(g * 128 + j, 16, stride=8), :] = summed
            for h in range(2):
                rows = slice(h * 16, (h + 1) * 16)
                stats = jnp.where(lane == h * 8 + j, peak[rows], stats)
                stats = jnp.where(lane == 16 + h * 8 + j, total[rows], stats)
        stat[g * 16 : (g + 1) * 16, :] = stats
        numb[here, :] = num[here, :].astype(BF16)

        def num_of(to_x, to_p, g=g):
            at = g * 128 + ((to_p % 2) * 4 + to_x) * 16
            return numb.at[pl.ds(pl.multiple_of(at, 16), 16), :]

        def stat_of(to_x, to_p, g=g):
            at = g * 16 + ((to_p % 2) * 4 + to_x) * 2
            return stat.at[pl.ds(pl.multiple_of(at, 2), 2), :]

        group = [t for t in PARTNERS if t[1] == dy]
        send_plane(stat_of, r6s.at[q], 5, group)
        send_plane(num_of, r6.at[q], 4, group)
    own_at = 3 * 128 + (c * 4 + x) * 16
    r6[q] = numb[pl.ds(pl.multiple_of(own_at, 16), 16), :]
    r6s[q] = stat[pl.ds(pl.multiple_of(48 + (c * 4 + x) * 2, 2), 2), :]
    l_co.wait()
    await_plane(r6s, 5)
    stats = jnp.concatenate(
        [r6s[...].reshape(64, 128), jnp.zeros((64, 128), F32)], axis=0
    ).T
    lane8 = lax.broadcasted_iota(jnp.int32, (8, 128), 1)
    shares = []
    for r in range(2):
        valid = (lane8 < 64) & (lane8 % 2 == r)
        pair = []
        for h in range(2):
            peaks = jnp.where(valid, stats[h * 8 : (h + 1) * 8, :], NEG)
            totals = stats[16 + h * 8 : 16 + (h + 1) * 8, :]
            scale = jnp.where(valid, jnp.exp(peaks - jnp.max(peaks, axis=1, keepdims=True)), 0.0)
            pair.append((scale, jnp.sum(scale * totals, axis=1, keepdims=True)))
        shares.append(pair)
    await_plane(r6, 4)
    low = lane8 < 64
    for r in range(2):
        (scale0, total0), (scale1, total1) = shares[r]
        terms = []
        for s in range(PLANE):
            at = slice(2 * s + r, 2 * s + r + 1)
            scale = jnp.where(low, scale0[:, at], scale1[:, at])
            terms.append(r6[s].astype(F32)[r * 8 : (r + 1) * 8, :] * scale)
        row_f[r * 8 : (r + 1) * 8, :] = tree(terms) / jnp.where(low, total0, total1)
    final = (back(dot(two_rows(), co[...])) + middle).astype(BF16)
    hid[...] = final
    r7[p] = final

    for dx, dy, dc in PARTNERS:
        if dx == 0:
            pltpu.make_async_remote_copy(
                src_ref=hid,
                dst_ref=r7.at[p],
                send_sem=send_sem.at[6],
                recv_sem=recv_sem.at[6],
                device_id=(d, ys[dy] * 2 + cs[dc]),
                device_id_type=MESH,
            ).start()
    for n, ref in enumerate((r1, r2, r4, r5, r6, r6s)):
        await_bytes(ref.at[pl.ds(0, 31)], send_sem.at[n])
    await_bytes(r7.at[pl.ds(0, PATCH - 1)], recv_sem.at[6])
    hidf[...] = r7[...].astype(F32).reshape(128, 128)
    for j in range(CHUNKS):
        hidden_ref[:, j * 128 : (j + 1) * 128] = hidf[pl.ds(j, 16, stride=8), :].astype(BF16)
    await_bytes(r7.at[pl.ds(0, PATCH - 1)], send_sem.at[6])


def emit(hidden, new_k, new_v, hidden_ref, newk_ref, newv_ref):
    hidden_ref[...] = hidden[...]
    newk_ref[...] = new_k[...]
    newv_ref[...] = new_v[...]


def shards(
    token_ids,
    parents,
    embedding,
    self_gain,
    query_weight,
    key_weight,
    value_weight,
    output_weight,
    past_keys,
    past_values,
    cross_gain,
    cross_query,
    cross_output,
    image_keys,
    image_values,
):
    vmem = pl.BlockSpec(memory_space=pltpu.VMEM)
    hbm = pl.BlockSpec(memory_space=pl.ANY)
    shapes = ((16, D), (16, 128), (16, 128))
    results = pl.pallas_call(
        kernel,
        out_shape=tuple(pltpu.VMEM(shape, BF16) for shape in shapes),
        in_specs=[hbm] * 15,
        out_specs=(vmem, vmem, vmem),
        scratch_shapes=[
            pltpu.VMEM((4, 128), jnp.int32),
            pltpu.VMEM((4, 128), jnp.int32),
            pltpu.VMEM((8, 128), BF16),
            pltpu.VMEM((8, 128), BF16),
            pltpu.VMEM((1024, 128), BF16),
            pltpu.VMEM((D, 384), BF16),
            pltpu.VMEM((128, D), BF16),
            pltpu.VMEM((2048, 128), BF16),
            pltpu.VMEM((2048, 128), BF16),
            pltpu.VMEM((D, D), BF16),
            pltpu.VMEM((D, D), BF16),
            pltpu.VMEM((512, D), BF16),
            pltpu.VMEM((512, D), BF16),
            pltpu.VMEM((512, D), BF16),
            pltpu.VMEM((512, 128), BF16),
            pltpu.VMEM((DP, 16, 128), BF16),
            pltpu.VMEM((16, 128), BF16),
            pltpu.VMEM((PLANE, 16, 128), BF16),
            pltpu.VMEM((512, 128), F32),
            pltpu.VMEM((256, 128), BF16),
            pltpu.VMEM((512, 128), F32),
            pltpu.VMEM((512, 128), BF16),
            pltpu.VMEM((PLANE, 16, 128), BF16),
            pltpu.VMEM((64, 128), F32),
            pltpu.VMEM((16, 128), BF16),
            pltpu.VMEM((PLANE, 16, 128), BF16),
            pltpu.VMEM((512, 128), F32),
            pltpu.VMEM((512, 128), F32),
            pltpu.VMEM((512, 128), BF16),
            pltpu.VMEM((PLANE, 16, 128), BF16),
            pltpu.VMEM((ROWS, 128), F32),
            pltpu.VMEM((PLANE, 2, 128), F32),
            pltpu.VMEM((16, 128), BF16),
            pltpu.VMEM((PATCH, 16, 128), BF16),
            pltpu.VMEM((128, 128), F32),
            pltpu.SemaphoreType.DMA((15,)),
            pltpu.SemaphoreType.DMA((7,)),
            pltpu.SemaphoreType.DMA((7,)),
            pltpu.SemaphoreType.REGULAR((8,)),
            pltpu.SemaphoreType.REGULAR,
        ],
        compiler_params=pltpu.CompilerParams(collective_id=0, has_side_effects=True),
        name="step",
    )(
        token_ids.reshape(4, 128),
        parents.reshape(4, 128),
        embedding,
        self_gain.reshape(8, 128),
        query_weight,
        key_weight,
        value_weight,
        output_weight,
        past_keys.reshape(2048, 128),
        past_values.reshape(2048, 128),
        cross_gain.reshape(8, 128),
        cross_query,
        cross_output,
        image_keys.reshape(512, D),
        image_values.reshape(512, D),
    )
    return pl.pallas_call(
        emit,
        out_shape=tuple(jax.ShapeDtypeStruct(shape, BF16) for shape in shapes),
        in_specs=[vmem] * 3,
        out_specs=(vmem, vmem, vmem),
        name="emit",
    )(*[pltpu.with_memory_space_constraint(r, pltpu.VMEM) for r in results])


def solution(mesh):
    in_specs = (
        P(),
        P(),
        P("dp", None),
        P(),
        P(None, "patch"),
        P(None, "patch"),
        P(None, "patch"),
        P("patch", None),
        P("dp", None, "patch"),
        P("dp", None, "patch"),
        P(),
        P(),
        P(),
        P("dp", None, "patch", None),
        P("dp", None, "patch", None),
    )
    out_specs = (P("dp", None), P("dp", "patch"), P("dp", "patch"))
    return jax.shard_map(
        shards, mesh=mesh, in_specs=in_specs, out_specs=out_specs, check_vma=False
    )
```

```python
import jax
import jax.numpy as jnp
from jax import lax
from jax.experimental import pallas as pl
from jax.experimental.pallas import tpu as pltpu
from jax.sharding import PartitionSpec as P

MESH = pl.DeviceIdType.MESH
F32 = jnp.float32
BF16 = jnp.bfloat16

D = 1024
CHUNKS = 8
BEAMS = 4
IMAGES = 16
ROWS = BEAMS * IMAGES
DP = 32
PATCH = 8
PLANE = 32
SLAB = 1000
LEN = 128
SPOTS = 32
NEG = -1e30
NT = (((1,), (1,)), ((), ()))


def dot(a, b):
    return jnp.dot(a, b, preferred_element_type=F32)


def dot_nt(a, b):
    return lax.dot_general(a, b, NT, preferred_element_type=F32)


def tree(parts):
    while len(parts) > 1:
        parts = [a + b for a, b in zip(parts[::2], parts[1::2])] + (
            [parts[-1]] if len(parts) % 2 else []
        )
    return parts[0]


def hops(step, size):
    return min(step, size - step)


PARTNERS = sorted(
    [(dx, dy, dc) for dx in range(4) for dy in range(4) for dc in range(2) if dx + dy + dc],
    key=lambda t: -hops(t[0], 4) - hops(t[1], 4),
)
ACROSS = (2, 1, 3, 0)


def split_heads(x):
    lane = lax.broadcasted_iota(jnp.int32, x.shape, 1)
    low = jnp.where(lane < 64, x, 0.0)
    high = jnp.where(lane < 64, 0.0, x)
    return jnp.concatenate([low, high], axis=0).astype(BF16)


def join_heads(x):
    half = x.shape[0] // 2
    lane = lax.broadcasted_iota(jnp.int32, (half, 128), 1)
    return jnp.where(lane < 64, x[:half], x[half:])


def kernel(
    ids_hbm,
    parents_hbm,
    emb_ref,
    sgain_hbm,
    wq_ref,
    wk_ref,
    wv_ref,
    wo_ref,
    pk_ref,
    pv_ref,
    cgain_hbm,
    cq_ref,
    co_ref,
    ik_ref,
    iv_ref,
    hidden_ref,
    newk_ref,
    newv_ref,
    ids_ref,
    parents_ref,
    sgain_ref,
    cgain_ref,
    emb,
    wqkv,
    wo,
    pk,
    pv,
    cq,
    co,
    ik,
    iv,
    onehot,
    owned,
    r1,
    tokc,
    r2,
    tokf,
    part,
    partb,
    r4,
    row_f,
    prob,
    r5,
    probf,
    num,
    numb,
    r6,
    stat,
    r6s,
    hid,
    r7,
    hidf,
    load_sem,
    send_sem,
    recv_sem,
    ready,
    in_plane,
):
    d = lax.axis_index("dp")
    p = lax.axis_index("patch")
    z, x = d // 4, d % 4
    y, c = p // 2, p % 2
    q = x * 8 + p
    zs = [lax.rem(z + k, 8) for k in range(8)]
    xs = [lax.rem(x + k, 4) for k in range(4)]
    ys = [lax.rem(y + k, 4) for k in range(4)]
    cs = [c, 1 - c]

    loads = []

    def load(src, dst):
        copy = pltpu.make_async_copy(src, dst, load_sem.at[len(loads)])
        copy.start()
        loads.append(copy)
        return copy

    emb[992:1024, :] = jnp.zeros((32, 128), BF16)
    l_ids = load(ids_hbm, ids_ref)
    l_emb = load(emb_ref.at[:, pl.ds(pl.multiple_of(p * 128, 128), 128)], emb.at[pl.ds(0, SLAB), :])

    barrier = pltpu.get_barrier_semaphore()

    def signal(sem, device):
        pl.semaphore_signal(sem, inc=1, device_id=device, device_id_type=MESH)

    ps = [lax.rem(p + k, 8) for k in range(8)]

    def later(of_z, of_plane):
        for dz in range(1, 8):

            @pl.when(z + dz < 8)
            def _(dz=dz):
                for dx in ACROSS:
                    signal(of_z, (zs[dz] * 4 + xs[dx], p))

        for dx in range(1, 4):

            @pl.when(x + dx < 4)
            def _(dx=dx):
                for k in range(8):
                    signal(of_plane, (z * 4 + xs[dx], ps[k]))

        for k in range(1, 8):

            @pl.when(p + k < 8)
            def _(k=k):
                signal(of_plane, (d, ps[k]))

    def earlier(of_z, of_plane):
        for dz in range(1, 8):

            @pl.when(z + dz >= 8)
            def _(dz=dz):
                for dx in ACROSS:
                    signal(of_z, (zs[dz] * 4 + xs[dx], p))

        for dx in range(1, 4):

            @pl.when(x + dx >= 4)
            def _(dx=dx):
                for k in range(8):
                    signal(of_plane, (z * 4 + xs[dx], ps[k]))

        for k in range(1, 8):

            @pl.when(p + k >= 8)
            def _(k=k):
                signal(of_plane, (d, ps[k]))

    later(barrier, barrier)

    l_q = load(wq_ref, wqkv.at[:, 0:128])
    l_k = load(wk_ref, wqkv.at[:, 128:256])
    l_v = load(wv_ref, wqkv.at[:, 256:384])
    l_gain = load(sgain_hbm, sgain_ref)
    l_parents = load(parents_hbm, parents_ref)
    l_pk = load(pk_ref, pk)
    l_pv = load(pv_ref, pv)
    l_wo = load(wo_ref, wo)
    l_cgain = load(cgain_hbm, cgain_ref)
    l_cq = load(cq_ref, cq)
    l_ik = load(ik_ref, ik)
    l_iv = load(iv_ref, iv)
    l_co = load(co_ref, co)

    @pl.when(4 * z + q > 0)
    def _():
        pl.semaphore_wait(barrier, 4 * z + q)

    earlier(ready.at[z], in_plane)

    row_f[...] = jnp.zeros((64, 128), F32)

    l_ids.wait()
    lane1024 = lax.broadcasted_iota(jnp.int32, (128, 1024), 1)
    for n in range(4):
        col = jnp.broadcast_to(ids_ref[n : n + 1, :], (128, 128)).T - d * SLAB
        wide = jnp.concatenate([col] * 8, axis=1)
        onehot[n * 128 : (n + 1) * 128, :] = jnp.where(wide == lane1024, 1.0, 0.0).astype(BF16)
    l_emb.wait()
    for n in range(4):
        rows = slice(n * 128, (n + 1) * 128)
        owned[rows, :] = dot(onehot[rows, :], emb[...]).astype(BF16)

    def await_bytes(ref, sem):
        pltpu.make_async_copy(ref, ref, sem).wait()

    def send1(dz, dx):
        to = zs[dz] * 4 + xs[dx]
        pltpu.make_async_remote_copy(
            src_ref=owned.at[pl.ds(pl.multiple_of(to * 16, 16), 16), :],
            dst_ref=r1.at[d],
            send_sem=send_sem.at[0],
            recv_sem=recv_sem.at[0],
            device_id=(to, p),
            device_id_type=MESH,
        ).start()

    for dz in (4, 3, 5, 2, 6, 1, 7):

        @pl.when(z + dz >= 8)
        def _(dz=dz):
            for dx in ACROSS:
                send1(dz, dx)


    @pl.when(q < PLANE - 1)
    def _():
        pl.semaphore_wait(in_plane, (PLANE - 1) - q)

    for dx in ACROSS[:3]:
        send1(0, dx)
    for dz in range(1, 8):

        @pl.when(z + dz < 8)
        def _(dz=dz):
            pl.semaphore_wait(ready.at[zs[dz]], 4)
            for dx in ACROSS:
                send1(dz, dx)

    r1[d] = owned[pl.ds(pl.multiple_of(d * 16, 16), 16), :]
    await_bytes(r1.at[pl.ds(0, DP - 1)], recv_sem.at[0])
    chunk = tree([r1[s] for s in range(DP)])
    tokc[...] = chunk
    r2[q] = chunk

    def send_plane(src_of, dst, n):
        for dx, dy, dc in PARTNERS:
            to_x, to_p = xs[dx], ys[dy] * 2 + cs[dc]
            pltpu.make_async_remote_copy(
                src_ref=src_of(to_x, to_p),
                dst_ref=dst,
                send_sem=send_sem.at[n],
                recv_sem=recv_sem.at[n],
                device_id=(z * 4 + to_x, to_p),
                device_id_type=MESH,
            ).start()

    def await_plane(dst, n):
        await_bytes(dst.at[pl.ds(0, PLANE - 1)], recv_sem.at[n])

    send_plane(lambda to_x, to_p: tokc, r2.at[q], 1)
    l_q.wait()
    l_k.wait()
    l_v.wait()
    l_gain.wait()
    await_plane(r2, 1)

    toks = [
        jnp.concatenate([r2[b * 8 + j] for b in range(BEAMS)], axis=0).astype(F32)
        for j in range(CHUNKS)
    ]
    for j in range(CHUNKS):
        tokf[pl.ds(j, ROWS, stride=8), :] = toks[j]
    square = tree([t * t for t in toks])
    factor = lax.rsqrt(jnp.sum(square, axis=1, keepdims=True) * (1.0 / D) + 1e-06)
    sgain = sgain_ref[...].astype(F32)
    normed = jnp.concatenate(
        [(toks[j] * factor * sgain[j : j + 1, :]).astype(BF16) for j in range(CHUNKS)], axis=1
    )
    qkv = dot(normed, wqkv[...]).astype(BF16)
    new_q, new_k, new_v = (qkv[:, n * 128 : (n + 1) * 128].astype(F32) for n in range(3))
    queries = split_heads(new_q)
    own = jnp.sum(
        queries.astype(F32) * jnp.concatenate([new_k, new_k], axis=0), axis=1, keepdims=True
    )
    own = own * 0.125
    hidf[0:ROWS, :] = new_k
    hidf[ROWS : 2 * ROWS, :] = new_v
    newk_ref[...] = hidf[pl.ds(pl.multiple_of(x * 16, 16), 16), :].astype(BF16)
    newv_ref[...] = hidf[pl.ds(pl.multiple_of(ROWS + x * 16, 16), 16), :].astype(BF16)

    by_image = [pl.ds(i, 8, stride=16) for i in range(IMAGES)]
    hidf[...] = queries.astype(F32)
    l_pk.wait()
    parts = [
        dot_nt(hidf[by_image[i], :].astype(BF16), pk[i * LEN : (i + 1) * LEN, :])
        for i in range(IMAGES)
    ]
    for i in range(IMAGES):
        hidf[by_image[i], :] = parts[i]
    scores = hidf[...] * 0.125
    peak = jnp.maximum(jnp.max(scores, axis=1, keepdims=True), own)
    powers = jnp.exp(scores - peak)
    own_power = jnp.exp(own - peak)
    total = jnp.sum(powers, axis=1, keepdims=True) + own_power
    own_weight = own_power.astype(BF16).astype(F32)
    hidf[...] = powers
    l_pv.wait()
    parts = [
        dot(hidf[by_image[i], :].astype(BF16), pv[i * LEN : (i + 1) * LEN, :])
        for i in range(IMAGES)
    ]
    for i in range(IMAGES):
        hidf[by_image[i], :] = parts[i]
    context = hidf[...]
    context = (context + own_weight * jnp.concatenate([new_v, new_v], axis=0)) / total
    context = join_heads(context)
    l_parents.wait()
    pcol = jnp.broadcast_to(parents_ref[pl.ds(z // 2, 1), :], (128, 128)).T
    pcol = jnp.where(z % 2 == 0, pcol[:ROWS], pcol[ROWS:])
    context = jnp.where(pcol == x, context, 0.0).astype(BF16)

    l_wo.wait()
    projected = dot(context, wo[...])
    for j in range(CHUNKS):
        part[pl.ds(j, ROWS, stride=8), :] = projected[:, j * 128 : (j + 1) * 128]
    partb[...] = part[...].astype(BF16)
    mine = pl.ds(pl.multiple_of(q * 16, 16), 16)

    def part_of(to_x, to_p):
        return partb.at[pl.ds(pl.multiple_of((to_x * 8 + to_p) * 16, 16), 16), :]

    send_plane(part_of, r4.at[q], 2)
    r4[q] = partb[mine, :]
    l_cgain.wait()
    l_cq.wait()
    await_plane(r4, 2)
    middle = tree([r4[s].astype(F32) for s in range(PLANE)]) + tokf[mine, :]

    cgain = cgain_ref[...].astype(F32)
    for r in range(2):
        row = middle[r * 8 : (r + 1) * 8, :]
        factor = lax.rsqrt(jnp.sum(row * row, keepdims=True) * (1.0 / D) + 1e-06)
        row_f[r * 8 : (r + 1) * 8, :] = row * factor * cgain

    def two_rows():
        return jnp.concatenate(
            [row_f[pl.ds(j, 8, stride=8), :] for j in range(CHUNKS)], axis=1
        ).astype(BF16)

    def back(value):
        for j in range(CHUNKS):
            row_f[pl.ds(j, 8, stride=8), :] = value[:, j * 128 : (j + 1) * 128]
        return row_f[0:16, :]

    mine_probe = back(dot(two_rows(), cq[...])).astype(BF16)
    prob[...] = mine_probe
    slot = p * 4 + x
    r5[slot] = mine_probe

    send_plane(lambda to_x, to_p: prob, r5.at[slot], 3)
    l_ik.wait()
    l_iv.wait()
    await_plane(r5, 3)

    probf[...] = r5[...].astype(F32).reshape(512, 128)
    units = [
        (slice(g * 128, (g + 1) * 128), slice(j * 128, (j + 1) * 128), pl.ds(g * 128 + j, 16, stride=8))
        for g in range(4)
        for j in range(CHUNKS)
    ]
    scores = jnp.concatenate(
        [dot_nt(split_heads(probf[rows, :]), ik[keys, block]) for keys, block, rows in units], axis=0
    )
    row = lax.broadcasted_iota(jnp.int32, scores.shape, 0)
    image = (row // 8 % 2) * 2 + row % 2
    same = image == lax.broadcasted_iota(jnp.int32, scores.shape, 1) // SPOTS
    scores = jnp.where(same, scores * 0.125, NEG)
    peak = jnp.max(scores, axis=1, keepdims=True)
    powers = jnp.exp(scores - peak)
    total = jnp.sum(powers, axis=1, keepdims=True)
    powers = powers.astype(BF16)
    lane = lax.broadcasted_iota(jnp.int32, (16, 128), 1)
    for g in range(4):
        stats = jnp.zeros((16, 128), F32)
        for j in range(CHUNKS):
            for h in range(2):
                at = (g * CHUNKS + j) * 32 + h * 16
                stats = jnp.where(lane == h * 8 + j, peak[at : at + 16], stats)
                stats = jnp.where(lane == 16 + h * 8 + j, total[at : at + 16], stats)
        stat[g * 16 : (g + 1) * 16, :] = stats
    for n, (keys, block, rows) in enumerate(units):
        num[rows, :] = join_heads(dot(powers[n * 32 : (n + 1) * 32], iv[keys, block]))
    numb[...] = num[...].astype(BF16)

    def num_of(to_x, to_p):
        return numb.at[pl.ds(pl.multiple_of((to_p * 4 + to_x) * 16, 16), 16), :]

    def stat_of(to_x, to_p):
        return stat.at[pl.ds(pl.multiple_of((to_p * 4 + to_x) * 2, 2), 2), :]

    send_plane(stat_of, r6s.at[q], 5)
    send_plane(num_of, r6.at[q], 4)
    r6[q] = numb[pl.ds(pl.multiple_of(slot * 16, 16), 16), :]
    r6s[q] = stat[pl.ds(pl.multiple_of(slot * 2, 2), 2), :]
    l_co.wait()
    await_plane(r6s, 5)
    stats = jnp.concatenate(
        [r6s[...].reshape(64, 128), jnp.zeros((64, 128), F32)], axis=0
    ).T
    lane8 = lax.broadcasted_iota(jnp.int32, (8, 128), 1)
    shares = []
    for r in range(2):
        valid = (lane8 < 64) & (lane8 % 2 == r)
        pair = []
        for h in range(2):
            peaks = jnp.where(valid, stats[h * 8 : (h + 1) * 8, :], NEG)
            totals = stats[16 + h * 8 : 16 + (h + 1) * 8, :]
            scale = jnp.where(valid, jnp.exp(peaks - jnp.max(peaks, axis=1, keepdims=True)), 0.0)
            pair.append((scale, jnp.sum(scale * totals, axis=1, keepdims=True)))
        shares.append(pair)
    await_plane(r6, 4)
    low = lane8 < 64
    for r in range(2):
        (scale0, total0), (scale1, total1) = shares[r]
        terms = []
        for s in range(PLANE):
            at = slice(2 * s + r, 2 * s + r + 1)
            scale = jnp.where(low, scale0[:, at], scale1[:, at])
            terms.append(r6[s].astype(F32)[r * 8 : (r + 1) * 8, :] * scale)
        row_f[r * 8 : (r + 1) * 8, :] = tree(terms) / jnp.where(low, total0, total1)
    final = (back(dot(two_rows(), co[...])) + middle).astype(BF16)
    hid[...] = final
    r7[p] = final

    for dx, dy, dc in PARTNERS:
        if dx == 0:
            pltpu.make_async_remote_copy(
                src_ref=hid,
                dst_ref=r7.at[p],
                send_sem=send_sem.at[6],
                recv_sem=recv_sem.at[6],
                device_id=(d, ys[dy] * 2 + cs[dc]),
                device_id_type=MESH,
            ).start()
    for n, ref in enumerate((r1, r2, r4, r5, r6, r6s)):
        await_bytes(ref.at[pl.ds(0, 31)], send_sem.at[n])
    await_bytes(r7.at[pl.ds(0, PATCH - 1)], recv_sem.at[6])
    hidf[...] = r7[...].astype(F32).reshape(128, 128)
    for j in range(CHUNKS):
        hidden_ref[:, j * 128 : (j + 1) * 128] = hidf[pl.ds(j, 16, stride=8), :].astype(BF16)
    await_bytes(r7.at[pl.ds(0, PATCH - 1)], send_sem.at[6])


def emit(hidden, new_k, new_v, hidden_ref, newk_ref, newv_ref):
    hidden_ref[...] = hidden[...]
    newk_ref[...] = new_k[...]
    newv_ref[...] = new_v[...]


def shards(
    token_ids,
    parents,
    embedding,
    self_gain,
    query_weight,
    key_weight,
    value_weight,
    output_weight,
    past_keys,
    past_values,
    cross_gain,
    cross_query,
    cross_output,
    image_keys,
    image_values,
):
    vmem = pl.BlockSpec(memory_space=pltpu.VMEM)
    hbm = pl.BlockSpec(memory_space=pl.ANY)
    shapes = ((16, D), (16, 128), (16, 128))
    results = pl.pallas_call(
        kernel,
        out_shape=tuple(pltpu.VMEM(shape, BF16) for shape in shapes),
        in_specs=[hbm] * 15,
        out_specs=(vmem, vmem, vmem),
        scratch_shapes=[
            pltpu.VMEM((4, 128), jnp.int32),
            pltpu.VMEM((4, 128), jnp.int32),
            pltpu.VMEM((8, 128), BF16),
            pltpu.VMEM((8, 128), BF16),
            pltpu.VMEM((1024, 128), BF16),
            pltpu.VMEM((D, 384), BF16),
            pltpu.VMEM((128, D), BF16),
            pltpu.VMEM((2048, 128), BF16),
            pltpu.VMEM((2048, 128), BF16),
            pltpu.VMEM((D, D), BF16),
            pltpu.VMEM((D, D), BF16),
            pltpu.VMEM((512, D), BF16),
            pltpu.VMEM((512, D), BF16),
            pltpu.VMEM((512, D), BF16),
            pltpu.VMEM((512, 128), BF16),
            pltpu.VMEM((DP, 16, 128), BF16),
            pltpu.VMEM((16, 128), BF16),
            pltpu.VMEM((PLANE, 16, 128), BF16),
            pltpu.VMEM((512, 128), F32),
            pltpu.VMEM((512, 128), F32),
            pltpu.VMEM((512, 128), BF16),
            pltpu.VMEM((PLANE, 16, 128), BF16),
            pltpu.VMEM((64, 128), F32),
            pltpu.VMEM((16, 128), BF16),
            pltpu.VMEM((PLANE, 16, 128), BF16),
            pltpu.VMEM((512, 128), F32),
            pltpu.VMEM((512, 128), F32),
            pltpu.VMEM((512, 128), BF16),
            pltpu.VMEM((PLANE, 16, 128), BF16),
            pltpu.VMEM((ROWS, 128), F32),
            pltpu.VMEM((PLANE, 2, 128), F32),
            pltpu.VMEM((16, 128), BF16),
            pltpu.VMEM((PATCH, 16, 128), BF16),
            pltpu.VMEM((128, 128), F32),
            pltpu.SemaphoreType.DMA((15,)),
            pltpu.SemaphoreType.DMA((7,)),
            pltpu.SemaphoreType.DMA((7,)),
            pltpu.SemaphoreType.REGULAR((8,)),
            pltpu.SemaphoreType.REGULAR,
        ],
        compiler_params=pltpu.CompilerParams(collective_id=0, has_side_effects=True),
        name="step",
    )(
        token_ids.reshape(4, 128),
        parents.reshape(4, 128),
        embedding,
        self_gain.reshape(8, 128),
        query_weight,
        key_weight,
        value_weight,
        output_weight,
        past_keys.reshape(2048, 128),
        past_values.reshape(2048, 128),
        cross_gain.reshape(8, 128),
        cross_query,
        cross_output,
        image_keys.reshape(512, D),
        image_values.reshape(512, D),
    )
    return pl.pallas_call(
        emit,
        out_shape=tuple(jax.ShapeDtypeStruct(shape, BF16) for shape in shapes),
        in_specs=[vmem] * 3,
        out_specs=(vmem, vmem, vmem),
        name="emit",
    )(*[pltpu.with_memory_space_constraint(r, pltpu.VMEM) for r in results])


def solution(mesh):
    in_specs = (
        P(),
        P(),
        P("dp", None),
        P(),
        P(None, "patch"),
        P(None, "patch"),
        P(None, "patch"),
        P("patch", None),
        P("dp", None, "patch"),
        P("dp", None, "patch"),
        P(),
        P(),
        P(),
        P("dp", None, "patch", None),
        P("dp", None, "patch", None),
    )
    out_specs = (P("dp", None), P("dp", "patch"), P("dp", "patch"))
    return jax.shard_map(
        shards, mesh=mesh, in_specs=in_specs, out_specs=out_specs, check_vma=False
    )
```

```python
import jax
import jax.numpy as jnp
from jax import lax
from jax.experimental import pallas as pl
from jax.experimental.pallas import tpu as pltpu
from jax.sharding import PartitionSpec as P

MESH = pl.DeviceIdType.MESH
F32 = jnp.float32
BF16 = jnp.bfloat16

D = 1024
CHUNKS = 8
BEAMS = 4
IMAGES = 16
ROWS = BEAMS * IMAGES
DP = 32
PATCH = 8
PLANE = 32
SLAB = 1000
LEN = 128
SPOTS = 32
NEG = -1e30
NT = (((1,), (1,)), ((), ()))


def dot(a, b):
    return jnp.dot(a, b, preferred_element_type=F32)


def dot_nt(a, b):
    return lax.dot_general(a, b, NT, preferred_element_type=F32)


def tree(parts):
    while len(parts) > 1:
        parts = [a + b for a, b in zip(parts[::2], parts[1::2])] + (
            [parts[-1]] if len(parts) % 2 else []
        )
    return parts[0]


def hops(step, size):
    return min(step, size - step)


PARTNERS = sorted(
    [(dx, dy, dc) for dx in range(4) for dy in range(4) for dc in range(2) if dx + dy + dc],
    key=lambda t: -hops(t[0], 4) - hops(t[1], 4),
)
ACROSS = (2, 1, 3, 0)


def split_heads(x):
    lane = lax.broadcasted_iota(jnp.int32, x.shape, 1)
    low = jnp.where(lane < 64, x, 0.0)
    high = jnp.where(lane < 64, 0.0, x)
    return jnp.concatenate([low, high], axis=0).astype(BF16)


def join_heads(x):
    half = x.shape[0] // 2
    lane = lax.broadcasted_iota(jnp.int32, (half, 128), 1)
    return jnp.where(lane < 64, x[:half], x[half:])


def kernel(
    ids_hbm,
    parents_hbm,
    emb_ref,
    sgain_hbm,
    wq_ref,
    wk_ref,
    wv_ref,
    wo_ref,
    pk_ref,
    pv_ref,
    cgain_hbm,
    cq_ref,
    co_ref,
    ik_ref,
    iv_ref,
    hidden_ref,
    newk_ref,
    newv_ref,
    ids_ref,
    parents_ref,
    sgain_ref,
    cgain_ref,
    emb,
    wqkv,
    wo,
    pk,
    pv,
    cq,
    co,
    ik,
    iv,
    onehot,
    owned,
    r1,
    tokc,
    r2,
    tokf,
    part,
    partb,
    r4,
    row_f,
    prob,
    r5,
    probf,
    num,
    numb,
    r6,
    stat,
    r6s,
    hid,
    r7,
    hidf,
    load_sem,
    send_sem,
    recv_sem,
    ready,
):
    d = lax.axis_index("dp")
    p = lax.axis_index("patch")
    z, x = d // 4, d % 4
    y, c = p // 2, p % 2
    q = x * 8 + p
    zs = [lax.rem(z + k, 8) for k in range(8)]
    xs = [lax.rem(x + k, 4) for k in range(4)]
    ys = [lax.rem(y + k, 4) for k in range(4)]
    cs = [c, 1 - c]

    loads = []

    def load(src, dst):
        copy = pltpu.make_async_copy(src, dst, load_sem.at[len(loads)])
        copy.start()
        loads.append(copy)
        return copy

    emb[992:1024, :] = jnp.zeros((32, 128), BF16)
    l_ids = load(ids_hbm, ids_ref)
    l_emb = load(emb_ref.at[:, pl.ds(pl.multiple_of(p * 128, 128), 128)], emb.at[pl.ds(0, SLAB), :])

    barrier = pltpu.get_barrier_semaphore()

    def signal(sem, device):
        pl.semaphore_signal(sem, inc=1, device_id=device, device_id_type=MESH)

    for dz in range(1, 8):

        @pl.when(z + dz < 8)
        def _(dz=dz):
            for dx in ACROSS:
                signal(barrier, (zs[dz] * 4 + xs[dx], p))

    for dx, dy, dc in PARTNERS:
        signal(barrier, (z * 4 + xs[dx], ys[dy] * 2 + cs[dc]))

    l_q = load(wq_ref, wqkv.at[:, 0:128])
    l_k = load(wk_ref, wqkv.at[:, 128:256])
    l_v = load(wv_ref, wqkv.at[:, 256:384])
    l_gain = load(sgain_hbm, sgain_ref)
    l_parents = load(parents_hbm, parents_ref)
    l_pk = load(pk_ref, pk)
    l_pv = load(pv_ref, pv)
    l_wo = load(wo_ref, wo)
    l_cgain = load(cgain_hbm, cgain_ref)
    l_cq = load(cq_ref, cq)
    l_ik = load(ik_ref, ik)
    l_iv = load(iv_ref, iv)
    l_co = load(co_ref, co)

    row_f[...] = jnp.zeros((64, 128), F32)

    l_ids.wait()
    lane1024 = lax.broadcasted_iota(jnp.int32, (128, 1024), 1)
    for n in range(4):
        col = jnp.broadcast_to(ids_ref[n : n + 1, :], (128, 128)).T - d * SLAB
        wide = jnp.concatenate([col] * 8, axis=1)
        onehot[n * 128 : (n + 1) * 128, :] = jnp.where(wide == lane1024, 1.0, 0.0).astype(BF16)
    l_emb.wait()
    for n in range(4):
        rows = slice(n * 128, (n + 1) * 128)
        owned[rows, :] = dot(onehot[rows, :], emb[...]).astype(BF16)

    pl.semaphore_wait(barrier, (PLANE - 1) + 4 * z)
    for dz in range(1, 8):

        @pl.when(z + dz >= 8)
        def _(dz=dz):
            for dx in ACROSS:
                signal(ready.at[z], (zs[dz] * 4 + xs[dx], p))

    def await_bytes(ref, sem):
        pltpu.make_async_copy(ref, ref, sem).wait()

    def send1(dz, dx):
        to = zs[dz] * 4 + xs[dx]
        pltpu.make_async_remote_copy(
            src_ref=owned.at[pl.ds(pl.multiple_of(to * 16, 16), 16), :],
            dst_ref=r1.at[d],
            send_sem=send_sem.at[0],
            recv_sem=recv_sem.at[0],
            device_id=(to, p),
            device_id_type=MESH,
        ).start()

    for dz in (4, 3, 5, 2, 6, 1, 7):

        @pl.when(z + dz >= 8)
        def _(dz=dz):
            for dx in ACROSS:
                send1(dz, dx)

    for dx in ACROSS[:3]:
        send1(0, dx)
    for dz in range(1, 8):

        @pl.when(z + dz < 8)
        def _(dz=dz):
            pl.semaphore_wait(ready.at[zs[dz]], 4)
            for dx in ACROSS:
                send1(dz, dx)

    r1[d] = owned[pl.ds(pl.multiple_of(d * 16, 16), 16), :]
    await_bytes(r1.at[pl.ds(0, DP - 1)], recv_sem.at[0])
    chunk = tree([r1[s] for s in range(DP)])
    tokc[...] = chunk
    r2[q] = chunk

    def send_plane(src_of, dst, n):
        for dx, dy, dc in PARTNERS:
            to_x, to_p = xs[dx], ys[dy] * 2 + cs[dc]
            pltpu.make_async_remote_copy(
                src_ref=src_of(to_x, to_p),
                dst_ref=dst,
                send_sem=send_sem.at[n],
                recv_sem=recv_sem.at[n],
                device_id=(z * 4 + to_x, to_p),
                device_id_type=MESH,
            ).start()

    def await_plane(dst, n):
        await_bytes(dst.at[pl.ds(0, PLANE - 1)], recv_sem.at[n])

    send_plane(lambda to_x, to_p: tokc, r2.at[q], 1)
    l_q.wait()
    l_k.wait()
    l_v.wait()
    l_gain.wait()
    await_plane(r2, 1)

    toks = [
        jnp.concatenate([r2[b * 8 + j] for b in range(BEAMS)], axis=0).astype(F32)
        for j in range(CHUNKS)
    ]
    for j in range(CHUNKS):
        tokf[pl.ds(j, ROWS, stride=8), :] = toks[j]
    square = tree([t * t for t in toks])
    factor = lax.rsqrt(jnp.sum(square, axis=1, keepdims=True) * (1.0 / D) + 1e-06)
    sgain = sgain_ref[...].astype(F32)
    normed = jnp.concatenate(
        [(toks[j] * factor * sgain[j : j + 1, :]).astype(BF16) for j in range(CHUNKS)], axis=1
    )
    qkv = dot(normed, wqkv[...]).astype(BF16)
    new_q, new_k, new_v = (qkv[:, n * 128 : (n + 1) * 128].astype(F32) for n in range(3))
    queries = split_heads(new_q)
    own = jnp.sum(
        queries.astype(F32) * jnp.concatenate([new_k, new_k], axis=0), axis=1, keepdims=True
    )
    own = own * 0.125
    hidf[0:ROWS, :] = new_k
    hidf[ROWS : 2 * ROWS, :] = new_v
    newk_ref[...] = hidf[pl.ds(pl.multiple_of(x * 16, 16), 16), :].astype(BF16)
    newv_ref[...] = hidf[pl.ds(pl.multiple_of(ROWS + x * 16, 16), 16), :].astype(BF16)

    by_image = [pl.ds(i, 8, stride=16) for i in range(IMAGES)]
    hidf[...] = queries.astype(F32)
    l_pk.wait()
    parts = [
        dot_nt(hidf[by_image[i], :].astype(BF16), pk[i * LEN : (i + 1) * LEN, :])
        for i in range(IMAGES)
    ]
    for i in range(IMAGES):
        hidf[by_image[i], :] = parts[i]
    scores = hidf[...] * 0.125
    peak = jnp.maximum(jnp.max(scores, axis=1, keepdims=True), own)
    powers = jnp.exp(scores - peak)
    own_power = jnp.exp(own - peak)
    total = jnp.sum(powers, axis=1, keepdims=True) + own_power
    own_weight = own_power.astype(BF16).astype(F32)
    hidf[...] = powers
    l_pv.wait()
    parts = [
        dot(hidf[by_image[i], :].astype(BF16), pv[i * LEN : (i + 1) * LEN, :])
        for i in range(IMAGES)
    ]
    for i in range(IMAGES):
        hidf[by_image[i], :] = parts[i]
    context = hidf[...]
    context = (context + own_weight * jnp.concatenate([new_v, new_v], axis=0)) / total
    context = join_heads(context)
    l_parents.wait()
    pcol = jnp.broadcast_to(parents_ref[pl.ds(z // 2, 1), :], (128, 128)).T
    pcol = jnp.where(z % 2 == 0, pcol[:ROWS], pcol[ROWS:])
    context = jnp.where(pcol == x, context, 0.0).astype(BF16)

    l_wo.wait()
    projected = dot(context, wo[...])
    for j in range(CHUNKS):
        part[pl.ds(j, ROWS, stride=8), :] = projected[:, j * 128 : (j + 1) * 128]
    partb[...] = part[...].astype(BF16)
    mine = pl.ds(pl.multiple_of(q * 16, 16), 16)

    def part_of(to_x, to_p):
        return partb.at[pl.ds(pl.multiple_of((to_x * 8 + to_p) * 16, 16), 16), :]

    send_plane(part_of, r4.at[q], 2)
    r4[q] = partb[mine, :]
    l_cgain.wait()
    l_cq.wait()
    await_plane(r4, 2)
    middle = tree([r4[s].astype(F32) for s in range(PLANE)]) + tokf[mine, :]

    cgain = cgain_ref[...].astype(F32)
    for r in range(2):
        row = middle[r * 8 : (r + 1) * 8, :]
        factor = lax.rsqrt(jnp.sum(row * row, keepdims=True) * (1.0 / D) + 1e-06)
        row_f[r * 8 : (r + 1) * 8, :] = row * factor * cgain

    def two_rows():
        return jnp.concatenate(
            [row_f[pl.ds(j, 8, stride=8), :] for j in range(CHUNKS)], axis=1
        ).astype(BF16)

    def back(value):
        for j in range(CHUNKS):
            row_f[pl.ds(j, 8, stride=8), :] = value[:, j * 128 : (j + 1) * 128]
        return row_f[0:16, :]

    mine_probe = back(dot(two_rows(), cq[...])).astype(BF16)
    prob[...] = mine_probe
    slot = p * 4 + x
    r5[slot] = mine_probe

    send_plane(lambda to_x, to_p: prob, r5.at[slot], 3)
    l_ik.wait()
    l_iv.wait()
    await_plane(r5, 3)

    probf[...] = r5[...].astype(F32).reshape(512, 128)
    units = [
        (slice(g * 128, (g + 1) * 128), slice(j * 128, (j + 1) * 128), pl.ds(g * 128 + j, 16, stride=8))
        for g in range(4)
        for j in range(CHUNKS)
    ]
    scores = jnp.concatenate(
        [dot_nt(split_heads(probf[rows, :]), ik[keys, block]) for keys, block, rows in units], axis=0
    )
    row = lax.broadcasted_iota(jnp.int32, scores.shape, 0)
    image = (row // 8 % 2) * 2 + row % 2
    same = image == lax.broadcasted_iota(jnp.int32, scores.shape, 1) // SPOTS
    scores = jnp.where(same, scores * 0.125, NEG)
    peak = jnp.max(scores, axis=1, keepdims=True)
    powers = jnp.exp(scores - peak)
    total = jnp.sum(powers, axis=1, keepdims=True)
    powers = powers.astype(BF16)
    lane = lax.broadcasted_iota(jnp.int32, (16, 128), 1)
    for g in range(4):
        stats = jnp.zeros((16, 128), F32)
        for j in range(CHUNKS):
            for h in range(2):
                at = (g * CHUNKS + j) * 32 + h * 16
                stats = jnp.where(lane == h * 8 + j, peak[at : at + 16], stats)
                stats = jnp.where(lane == 16 + h * 8 + j, total[at : at + 16], stats)
        stat[g * 16 : (g + 1) * 16, :] = stats
    for n, (keys, block, rows) in enumerate(units):
        num[rows, :] = join_heads(dot(powers[n * 32 : (n + 1) * 32], iv[keys, block]))
    numb[...] = num[...].astype(BF16)

    def num_of(to_x, to_p):
        return numb.at[pl.ds(pl.multiple_of((to_p * 4 + to_x) * 16, 16), 16), :]

    def stat_of(to_x, to_p):
        return stat.at[pl.ds(pl.multiple_of((to_p * 4 + to_x) * 2, 2), 2), :]

    send_plane(stat_of, r6s.at[q], 5)
    send_plane(num_of, r6.at[q], 4)
    r6[q] = numb[pl.ds(pl.multiple_of(slot * 16, 16), 16), :]
    r6s[q] = stat[pl.ds(pl.multiple_of(slot * 2, 2), 2), :]
    l_co.wait()
    await_plane(r6s, 5)
    stats = jnp.concatenate(
        [r6s[...].reshape(64, 128), jnp.zeros((64, 128), F32)], axis=0
    ).T
    lane8 = lax.broadcasted_iota(jnp.int32, (8, 128), 1)
    shares = []
    for r in range(2):
        valid = (lane8 < 64) & (lane8 % 2 == r)
        pair = []
        for h in range(2):
            peaks = jnp.where(valid, stats[h * 8 : (h + 1) * 8, :], NEG)
            totals = stats[16 + h * 8 : 16 + (h + 1) * 8, :]
            scale = jnp.where(valid, jnp.exp(peaks - jnp.max(peaks, axis=1, keepdims=True)), 0.0)
            pair.append((scale, jnp.sum(scale * totals, axis=1, keepdims=True)))
        shares.append(pair)
    await_plane(r6, 4)
    low = lane8 < 64
    for r in range(2):
        (scale0, total0), (scale1, total1) = shares[r]
        terms = []
        for s in range(PLANE):
            at = slice(2 * s + r, 2 * s + r + 1)
            scale = jnp.where(low, scale0[:, at], scale1[:, at])
            terms.append(r6[s].astype(F32)[r * 8 : (r + 1) * 8, :] * scale)
        row_f[r * 8 : (r + 1) * 8, :] = tree(terms) / jnp.where(low, total0, total1)
    final = (back(dot(two_rows(), co[...])) + middle).astype(BF16)
    hid[...] = final
    r7[p] = final

    for dx, dy, dc in PARTNERS:
        if dx == 0:
            pltpu.make_async_remote_copy(
                src_ref=hid,
                dst_ref=r7.at[p],
                send_sem=send_sem.at[6],
                recv_sem=recv_sem.at[6],
                device_id=(d, ys[dy] * 2 + cs[dc]),
                device_id_type=MESH,
            ).start()
    for n, ref in enumerate((r1, r2, r4, r5, r6, r6s)):
        await_bytes(ref.at[pl.ds(0, 31)], send_sem.at[n])
    await_bytes(r7.at[pl.ds(0, PATCH - 1)], recv_sem.at[6])
    hidf[...] = r7[...].astype(F32).reshape(128, 128)
    for j in range(CHUNKS):
        hidden_ref[:, j * 128 : (j + 1) * 128] = hidf[pl.ds(j, 16, stride=8), :].astype(BF16)
    await_bytes(r7.at[pl.ds(0, PATCH - 1)], send_sem.at[6])


def emit(hidden, new_k, new_v, hidden_ref, newk_ref, newv_ref):
    hidden_ref[...] = hidden[...]
    newk_ref[...] = new_k[...]
    newv_ref[...] = new_v[...]


def shards(
    token_ids,
    parents,
    embedding,
    self_gain,
    query_weight,
    key_weight,
    value_weight,
    output_weight,
    past_keys,
    past_values,
    cross_gain,
    cross_query,
    cross_output,
    image_keys,
    image_values,
):
    vmem = pl.BlockSpec(memory_space=pltpu.VMEM)
    hbm = pl.BlockSpec(memory_space=pl.ANY)
    shapes = ((16, D), (16, 128), (16, 128))
    results = pl.pallas_call(
        kernel,
        out_shape=tuple(pltpu.VMEM(shape, BF16) for shape in shapes),
        in_specs=[hbm] * 15,
        out_specs=(vmem, vmem, vmem),
        scratch_shapes=[
            pltpu.VMEM((4, 128), jnp.int32),
            pltpu.VMEM((4, 128), jnp.int32),
            pltpu.VMEM((8, 128), BF16),
            pltpu.VMEM((8, 128), BF16),
            pltpu.VMEM((1024, 128), BF16),
            pltpu.VMEM((D, 384), BF16),
            pltpu.VMEM((128, D), BF16),
            pltpu.VMEM((2048, 128), BF16),
            pltpu.VMEM((2048, 128), BF16),
            pltpu.VMEM((D, D), BF16),
            pltpu.VMEM((D, D), BF16),
            pltpu.VMEM((512, D), BF16),
            pltpu.VMEM((512, D), BF16),
            pltpu.VMEM((512, D), BF16),
            pltpu.VMEM((512, 128), BF16),
            pltpu.VMEM((DP, 16, 128), BF16),
            pltpu.VMEM((16, 128), BF16),
            pltpu.VMEM((PLANE, 16, 128), BF16),
            pltpu.VMEM((512, 128), F32),
            pltpu.VMEM((512, 128), F32),
            pltpu.VMEM((512, 128), BF16),
            pltpu.VMEM((PLANE, 16, 128), BF16),
            pltpu.VMEM((64, 128), F32),
            pltpu.VMEM((16, 128), BF16),
            pltpu.VMEM((PLANE, 16, 128), BF16),
            pltpu.VMEM((512, 128), F32),
            pltpu.VMEM((512, 128), F32),
            pltpu.VMEM((512, 128), BF16),
            pltpu.VMEM((PLANE, 16, 128), BF16),
            pltpu.VMEM((ROWS, 128), F32),
            pltpu.VMEM((PLANE, 2, 128), F32),
            pltpu.VMEM((16, 128), BF16),
            pltpu.VMEM((PATCH, 16, 128), BF16),
            pltpu.VMEM((128, 128), F32),
            pltpu.SemaphoreType.DMA((15,)),
            pltpu.SemaphoreType.DMA((7,)),
            pltpu.SemaphoreType.DMA((7,)),
            pltpu.SemaphoreType.REGULAR((8,)),
        ],
        compiler_params=pltpu.CompilerParams(collective_id=0, has_side_effects=True),
        name="step",
    )(
        token_ids.reshape(4, 128),
        parents.reshape(4, 128),
        embedding,
        self_gain.reshape(8, 128),
        query_weight,
        key_weight,
        value_weight,
        output_weight,
        past_keys.reshape(2048, 128),
        past_values.reshape(2048, 128),
        cross_gain.reshape(8, 128),
        cross_query,
        cross_output,
        image_keys.reshape(512, D),
        image_values.reshape(512, D),
    )
    return pl.pallas_call(
        emit,
        out_shape=tuple(jax.ShapeDtypeStruct(shape, BF16) for shape in shapes),
        in_specs=[vmem] * 3,
        out_specs=(vmem, vmem, vmem),
        name="emit",
    )(*[pltpu.with_memory_space_constraint(r, pltpu.VMEM) for r in results])


def solution(mesh):
    in_specs = (
        P(),
        P(),
        P("dp", None),
        P(),
        P(None, "patch"),
        P(None, "patch"),
        P(None, "patch"),
        P("patch", None),
        P("dp", None, "patch"),
        P("dp", None, "patch"),
        P(),
        P(),
        P(),
        P("dp", None, "patch", None),
        P("dp", None, "patch", None),
    )
    out_specs = (P("dp", None), P("dp", "patch"), P("dp", "patch"))
    return jax.shard_map(
        shards, mesh=mesh, in_specs=in_specs, out_specs=out_specs, check_vma=False
    )
```

```python
import jax
import jax.numpy as jnp
from jax import lax
from jax.experimental import pallas as pl
from jax.experimental.pallas import tpu as pltpu
from jax.sharding import PartitionSpec as P

MESH = pl.DeviceIdType.MESH
F32 = jnp.float32
BF16 = jnp.bfloat16

D = 1024
CHUNKS = 8
BEAMS = 4
IMAGES = 16
ROWS = BEAMS * IMAGES
DP = 32
PATCH = 8
PLANE = 32
SLAB = 1000
LEN = 128
SPOTS = 32
NEG = -1e30
NT = (((1,), (1,)), ((), ()))


def dot(a, b):
    return jnp.dot(a, b, preferred_element_type=F32)


def dot_nt(a, b):
    return lax.dot_general(a, b, NT, preferred_element_type=F32)


def tree(parts):
    while len(parts) > 1:
        parts = [a + b for a, b in zip(parts[::2], parts[1::2])] + (
            [parts[-1]] if len(parts) % 2 else []
        )
    return parts[0]


def hops(step, size):
    return min(step, size - step)


PARTNERS = sorted(
    [(dx, dy, dc) for dx in range(4) for dy in range(4) for dc in range(2) if dx + dy + dc],
    key=lambda t: -hops(t[0], 4) - hops(t[1], 4),
)
ACROSS = (2, 1, 3, 0)


def split_heads(x):
    lane = lax.broadcasted_iota(jnp.int32, x.shape, 1)
    low = jnp.where(lane < 64, x, 0.0)
    high = jnp.where(lane < 64, 0.0, x)
    return jnp.concatenate([low, high], axis=0).astype(BF16)


def join_heads(x):
    half = x.shape[0] // 2
    lane = lax.broadcasted_iota(jnp.int32, (half, 128), 1)
    return jnp.where(lane < 64, x[:half], x[half:])


def kernel(
    ids_hbm,
    parents_hbm,
    emb_ref,
    sgain_hbm,
    wq_ref,
    wk_ref,
    wv_ref,
    wo_ref,
    pk_ref,
    pv_ref,
    cgain_hbm,
    cq_ref,
    co_ref,
    ik_ref,
    iv_ref,
    hidden_ref,
    newk_ref,
    newv_ref,
    ids_ref,
    parents_ref,
    sgain_ref,
    cgain_ref,
    emb,
    wqkv,
    wo,
    pk,
    pv,
    cq,
    co,
    ik,
    iv,
    onehot,
    owned,
    r1,
    tokc,
    r2,
    tokf,
    part,
    partb,
    r4,
    row_f,
    prob,
    r5,
    probf,
    num,
    numb,
    r6,
    stat,
    r6s,
    hid,
    r7,
    hidf,
    load_sem,
    send_sem,
    recv_sem,
    ready,
):
    d = lax.axis_index("dp")
    p = lax.axis_index("patch")
    z, x = d // 4, d % 4
    y, c = p // 2, p % 2
    q = x * 8 + p
    zs = [lax.rem(z + k, 8) for k in range(8)]
    xs = [lax.rem(x + k, 4) for k in range(4)]
    ys = [lax.rem(y + k, 4) for k in range(4)]
    cs = [c, 1 - c]

    loads = []

    def load(src, dst):
        copy = pltpu.make_async_copy(src, dst, load_sem.at[len(loads)])
        copy.start()
        loads.append(copy)
        return copy

    emb[992:1024, :] = jnp.zeros((32, 128), BF16)
    l_ids = load(ids_hbm, ids_ref)
    l_emb = load(emb_ref.at[:, pl.ds(pl.multiple_of(p * 128, 128), 128)], emb.at[pl.ds(0, SLAB), :])

    barrier = pltpu.get_barrier_semaphore()

    def signal(sem, device):
        pl.semaphore_signal(sem, inc=1, device_id=device, device_id_type=MESH)

    for dz in range(1, 8):

        @pl.when(z + dz < 8)
        def _(dz=dz):
            for dx in ACROSS:
                signal(barrier, (zs[dz] * 4 + xs[dx], p))

    for dx, dy, dc in PARTNERS:
        signal(barrier, (z * 4 + xs[dx], ys[dy] * 2 + cs[dc]))

    l_q = load(wq_ref, wqkv.at[:, 0:128])
    l_k = load(wk_ref, wqkv.at[:, 128:256])
    l_v = load(wv_ref, wqkv.at[:, 256:384])
    l_gain = load(sgain_hbm, sgain_ref)
    l_parents = load(parents_hbm, parents_ref)
    l_pk = load(pk_ref, pk)
    l_pv = load(pv_ref, pv)
    l_wo = load(wo_ref, wo)
    l_cgain = load(cgain_hbm, cgain_ref)
    l_cq = load(cq_ref, cq)
    l_ik = load(ik_ref, ik)
    l_iv = load(iv_ref, iv)
    l_co = load(co_ref, co)

    row_f[...] = jnp.zeros((64, 128), F32)

    l_ids.wait()
    lane1024 = lax.broadcasted_iota(jnp.int32, (128, 1024), 1)
    for n in range(4):
        col = jnp.broadcast_to(ids_ref[n : n + 1, :], (128, 128)).T - d * SLAB
        wide = jnp.concatenate([col] * 8, axis=1)
        onehot[n * 128 : (n + 1) * 128, :] = jnp.where(wide == lane1024, 1.0, 0.0).astype(BF16)
    l_emb.wait()
    for n in range(4):
        rows = slice(n * 128, (n + 1) * 128)
        owned[rows, :] = dot(onehot[rows, :], emb[...]).astype(BF16)

    pl.semaphore_wait(barrier, (PLANE - 1) + 4 * z)
    for dz in range(1, 8):

        @pl.when(z + dz >= 8)
        def _(dz=dz):
            for dx in ACROSS:
                signal(ready.at[z], (zs[dz] * 4 + xs[dx], p))

    def await_bytes(ref, sem):
        pltpu.make_async_copy(ref, ref, sem).wait()

    def send1(dz, dx):
        to = zs[dz] * 4 + xs[dx]
        pltpu.make_async_remote_copy(
            src_ref=owned.at[pl.ds(pl.multiple_of(to * 16, 16), 16), :],
            dst_ref=r1.at[d],
            send_sem=send_sem.at[0],
            recv_sem=recv_sem.at[0],
            device_id=(to, p),
            device_id_type=MESH,
        ).start()

    for dz in (4, 3, 5, 2, 6, 1, 7):

        @pl.when(z + dz >= 8)
        def _(dz=dz):
            for dx in ACROSS:
                send1(dz, dx)

    for dx in ACROSS[:3]:
        send1(0, dx)
    for dz in range(1, 8):

        @pl.when(z + dz < 8)
        def _(dz=dz):
            pl.semaphore_wait(ready.at[zs[dz]], 4)
            for dx in ACROSS:
                send1(dz, dx)

    r1[d] = owned[pl.ds(pl.multiple_of(d * 16, 16), 16), :]
    await_bytes(r1.at[pl.ds(0, DP - 1)], recv_sem.at[0])
    chunk = tree([r1[s] for s in range(DP)])
    tokc[...] = chunk
    r2[q] = chunk

    def send_plane(src_of, dst, n):
        for dx, dy, dc in PARTNERS:
            to_x, to_p = xs[dx], ys[dy] * 2 + cs[dc]
            pltpu.make_async_remote_copy(
                src_ref=src_of(to_x, to_p),
                dst_ref=dst,
                send_sem=send_sem.at[n],
                recv_sem=recv_sem.at[n],
                device_id=(z * 4 + to_x, to_p),
                device_id_type=MESH,
            ).start()

    def await_plane(dst, n):
        await_bytes(dst.at[pl.ds(0, PLANE - 1)], recv_sem.at[n])

    send_plane(lambda to_x, to_p: tokc, r2.at[q], 1)
    l_q.wait()
    l_k.wait()
    l_v.wait()
    l_gain.wait()
    await_plane(r2, 1)

    toks = [
        jnp.concatenate([r2[b * 8 + j] for b in range(BEAMS)], axis=0).astype(F32)
        for j in range(CHUNKS)
    ]
    square = tree([t * t for t in toks])
    factor = lax.rsqrt(jnp.sum(square, axis=1, keepdims=True) * (1.0 / D) + 1e-06)
    sgain = sgain_ref[...].astype(F32)
    normed = jnp.concatenate(
        [(toks[j] * factor * sgain[j : j + 1, :]).astype(BF16) for j in range(CHUNKS)], axis=1
    )
    qkv = dot(normed, wqkv[...]).astype(BF16)
    new_q, new_k, new_v = (qkv[:, n * 128 : (n + 1) * 128].astype(F32) for n in range(3))
    queries = split_heads(new_q)
    own = jnp.sum(
        queries.astype(F32) * jnp.concatenate([new_k, new_k], axis=0), axis=1, keepdims=True
    )
    own = own * 0.125

    by_image = [pl.ds(i, 8, stride=16) for i in range(IMAGES)]
    hidf[...] = queries.astype(F32)
    l_pk.wait()
    parts = [
        dot_nt(hidf[by_image[i], :].astype(BF16), pk[i * LEN : (i + 1) * LEN, :])
        for i in range(IMAGES)
    ]
    for i in range(IMAGES):
        hidf[by_image[i], :] = parts[i]
    scores = hidf[...] * 0.125
    peak = jnp.maximum(jnp.max(scores, axis=1, keepdims=True), own)
    powers = jnp.exp(scores - peak)
    own_power = jnp.exp(own - peak)
    total = jnp.sum(powers, axis=1, keepdims=True) + own_power
    own_weight = own_power.astype(BF16).astype(F32)
    hidf[...] = powers
    l_pv.wait()
    parts = [
        dot(hidf[by_image[i], :].astype(BF16), pv[i * LEN : (i + 1) * LEN, :])
        for i in range(IMAGES)
    ]
    for i in range(IMAGES):
        hidf[by_image[i], :] = parts[i]
    context = hidf[...]
    context = (context + own_weight * jnp.concatenate([new_v, new_v], axis=0)) / total
    context = join_heads(context)
    l_parents.wait()
    pcol = jnp.broadcast_to(parents_ref[pl.ds(z // 2, 1), :], (128, 128)).T
    pcol = jnp.where(z % 2 == 0, pcol[:ROWS], pcol[ROWS:])
    context = jnp.where(pcol == x, context, 0.0).astype(BF16)

    l_wo.wait()
    projected = dot(context, wo[...])
    for j in range(CHUNKS):
        part[pl.ds(j, ROWS, stride=8), :] = projected[:, j * 128 : (j + 1) * 128]
    partb[...] = part[...].astype(BF16)
    mine = pl.ds(pl.multiple_of(q * 16, 16), 16)

    def part_of(to_x, to_p):
        return partb.at[pl.ds(pl.multiple_of((to_x * 8 + to_p) * 16, 16), 16), :]

    send_plane(part_of, r4.at[q], 2)
    r4[q] = partb[mine, :]
    hidf[0:ROWS, :] = new_k
    hidf[ROWS : 2 * ROWS, :] = new_v
    newk_ref[...] = hidf[pl.ds(pl.multiple_of(x * 16, 16), 16), :].astype(BF16)
    newv_ref[...] = hidf[pl.ds(pl.multiple_of(ROWS + x * 16, 16), 16), :].astype(BF16)
    for j in range(CHUNKS):
        tokf[pl.ds(j, 16, stride=8), :] = r2[x * 8 + j].astype(F32)
    l_cgain.wait()
    l_cq.wait()
    await_plane(r4, 2)
    middle = tree([r4[s].astype(F32) for s in range(PLANE)]) + tokf[pl.ds(pl.multiple_of(p * 16, 16), 16), :]

    cgain = cgain_ref[...].astype(F32)
    for r in range(2):
        row = middle[r * 8 : (r + 1) * 8, :]
        factor = lax.rsqrt(jnp.sum(row * row, keepdims=True) * (1.0 / D) + 1e-06)
        row_f[r * 8 : (r + 1) * 8, :] = row * factor * cgain

    def two_rows():
        return jnp.concatenate(
            [row_f[pl.ds(j, 8, stride=8), :] for j in range(CHUNKS)], axis=1
        ).astype(BF16)

    def back(value):
        for j in range(CHUNKS):
            row_f[pl.ds(j, 8, stride=8), :] = value[:, j * 128 : (j + 1) * 128]
        return row_f[0:16, :]

    mine_probe = back(dot(two_rows(), cq[...])).astype(BF16)
    prob[...] = mine_probe
    slot = p * 4 + x
    r5[slot] = mine_probe

    send_plane(lambda to_x, to_p: prob, r5.at[slot], 3)
    l_ik.wait()
    l_iv.wait()
    await_plane(r5, 3)

    probf[...] = r5[...].astype(F32).reshape(512, 128)
    units = [
        (slice(g * 128, (g + 1) * 128), slice(j * 128, (j + 1) * 128), pl.ds(g * 128 + j, 16, stride=8))
        for g in range(4)
        for j in range(CHUNKS)
    ]
    scores = jnp.concatenate(
        [dot_nt(split_heads(probf[rows, :]), ik[keys, block]) for keys, block, rows in units], axis=0
    )
    row = lax.broadcasted_iota(jnp.int32, scores.shape, 0)
    image = (row // 8 % 2) * 2 + row % 2
    same = image == lax.broadcasted_iota(jnp.int32, scores.shape, 1) // SPOTS
    scores = jnp.where(same, scores * 0.125, NEG)
    peak = jnp.max(scores, axis=1, keepdims=True)
    powers = jnp.exp(scores - peak)
    total = jnp.sum(powers, axis=1, keepdims=True)
    powers = powers.astype(BF16)
    lane = lax.broadcasted_iota(jnp.int32, (16, 128), 1)
    for g in range(4):
        stats = jnp.zeros((16, 128), F32)
        for j in range(CHUNKS):
            for h in range(2):
                at = (g * CHUNKS + j) * 32 + h * 16
                stats = jnp.where(lane == h * 8 + j, peak[at : at + 16], stats)
                stats = jnp.where(lane == 16 + h * 8 + j, total[at : at + 16], stats)
        stat[g * 16 : (g + 1) * 16, :] = stats
    def stat_of(to_x, to_p):
        return stat.at[pl.ds(pl.multiple_of((to_p * 4 + to_x) * 2, 2), 2), :]

    send_plane(stat_of, r6s.at[q], 5)
    for n, (keys, block, rows) in enumerate(units):
        num[rows, :] = join_heads(dot(powers[n * 32 : (n + 1) * 32], iv[keys, block]))
    numb[...] = num[...].astype(BF16)

    def num_of(to_x, to_p):
        return numb.at[pl.ds(pl.multiple_of((to_p * 4 + to_x) * 16, 16), 16), :]

    send_plane(num_of, r6.at[q], 4)
    r6[q] = numb[pl.ds(pl.multiple_of(slot * 16, 16), 16), :]
    r6s[q] = stat[pl.ds(pl.multiple_of(slot * 2, 2), 2), :]
    l_co.wait()
    await_plane(r6s, 5)
    stats = jnp.concatenate(
        [r6s[...].reshape(64, 128), jnp.zeros((64, 128), F32)], axis=0
    ).T
    lane8 = lax.broadcasted_iota(jnp.int32, (8, 128), 1)
    shares = []
    for r in range(2):
        valid = (lane8 < 64) & (lane8 % 2 == r)
        pair = []
        for h in range(2):
            peaks = jnp.where(valid, stats[h * 8 : (h + 1) * 8, :], NEG)
            totals = stats[16 + h * 8 : 16 + (h + 1) * 8, :]
            scale = jnp.where(valid, jnp.exp(peaks - jnp.max(peaks, axis=1, keepdims=True)), 0.0)
            pair.append((scale, jnp.sum(scale * totals, axis=1, keepdims=True)))
        shares.append(pair)
    await_plane(r6, 4)
    low = lane8 < 64
    for r in range(2):
        (scale0, total0), (scale1, total1) = shares[r]
        terms = []
        for s in range(PLANE):
            at = slice(2 * s + r, 2 * s + r + 1)
            scale = jnp.where(low, scale0[:, at], scale1[:, at])
            terms.append(r6[s].astype(F32)[r * 8 : (r + 1) * 8, :] * scale)
        row_f[r * 8 : (r + 1) * 8, :] = tree(terms) / jnp.where(low, total0, total1)
    final = (back(dot(two_rows(), co[...])) + middle).astype(BF16)
    hid[...] = final
    r7[p] = final

    for dx, dy, dc in PARTNERS:
        if dx == 0:
            pltpu.make_async_remote_copy(
                src_ref=hid,
                dst_ref=r7.at[p],
                send_sem=send_sem.at[6],
                recv_sem=recv_sem.at[6],
                device_id=(d, ys[dy] * 2 + cs[dc]),
                device_id_type=MESH,
            ).start()
    for n, ref in enumerate((r1, r2, r4, r5, r6, r6s)):
        await_bytes(ref.at[pl.ds(0, 31)], send_sem.at[n])
    await_bytes(r7.at[pl.ds(0, PATCH - 1)], recv_sem.at[6])
    hidf[...] = r7[...].astype(F32).reshape(128, 128)
    for j in range(CHUNKS):
        hidden_ref[:, j * 128 : (j + 1) * 128] = hidf[pl.ds(j, 16, stride=8), :].astype(BF16)
    await_bytes(r7.at[pl.ds(0, PATCH - 1)], send_sem.at[6])


def emit(hidden, new_k, new_v, hidden_ref, newk_ref, newv_ref):
    hidden_ref[...] = hidden[...]
    newk_ref[...] = new_k[...]
    newv_ref[...] = new_v[...]


def shards(
    token_ids,
    parents,
    embedding,
    self_gain,
    query_weight,
    key_weight,
    value_weight,
    output_weight,
    past_keys,
    past_values,
    cross_gain,
    cross_query,
    cross_output,
    image_keys,
    image_values,
):
    vmem = pl.BlockSpec(memory_space=pltpu.VMEM)
    hbm = pl.BlockSpec(memory_space=pl.ANY)
    shapes = ((16, D), (16, 128), (16, 128))
    results = pl.pallas_call(
        kernel,
        out_shape=tuple(pltpu.VMEM(shape, BF16) for shape in shapes),
        in_specs=[hbm] * 15,
        out_specs=(vmem, vmem, vmem),
        scratch_shapes=[
            pltpu.VMEM((4, 128), jnp.int32),
            pltpu.VMEM((4, 128), jnp.int32),
            pltpu.VMEM((8, 128), BF16),
            pltpu.VMEM((8, 128), BF16),
            pltpu.VMEM((1024, 128), BF16),
            pltpu.VMEM((D, 384), BF16),
            pltpu.VMEM((128, D), BF16),
            pltpu.VMEM((2048, 128), BF16),
            pltpu.VMEM((2048, 128), BF16),
            pltpu.VMEM((D, D), BF16),
            pltpu.VMEM((D, D), BF16),
            pltpu.VMEM((512, D), BF16),
            pltpu.VMEM((512, D), BF16),
            pltpu.VMEM((512, D), BF16),
            pltpu.VMEM((512, 128), BF16),
            pltpu.VMEM((DP, 16, 128), BF16),
            pltpu.VMEM((16, 128), BF16),
            pltpu.VMEM((PLANE, 16, 128), BF16),
            pltpu.VMEM((128, 128), F32),
            pltpu.VMEM((512, 128), F32),
            pltpu.VMEM((512, 128), BF16),
            pltpu.VMEM((PLANE, 16, 128), BF16),
            pltpu.VMEM((64, 128), F32),
            pltpu.VMEM((16, 128), BF16),
            pltpu.VMEM((PLANE, 16, 128), BF16),
            pltpu.VMEM((512, 128), F32),
            pltpu.VMEM((512, 128), F32),
            pltpu.VMEM((512, 128), BF16),
            pltpu.VMEM((PLANE, 16, 128), BF16),
            pltpu.VMEM((ROWS, 128), F32),
            pltpu.VMEM((PLANE, 2, 128), F32),
            pltpu.VMEM((16, 128), BF16),
            pltpu.VMEM((PATCH, 16, 128), BF16),
            pltpu.VMEM((128, 128), F32),
            pltpu.SemaphoreType.DMA((15,)),
            pltpu.SemaphoreType.DMA((7,)),
            pltpu.SemaphoreType.DMA((7,)),
            pltpu.SemaphoreType.REGULAR((8,)),
        ],
        compiler_params=pltpu.CompilerParams(collective_id=0, has_side_effects=True),
        name="step",
    )(
        token_ids.reshape(4, 128),
        parents.reshape(4, 128),
        embedding,
        self_gain.reshape(8, 128),
        query_weight,
        key_weight,
        value_weight,
        output_weight,
        past_keys.reshape(2048, 128),
        past_values.reshape(2048, 128),
        cross_gain.reshape(8, 128),
        cross_query,
        cross_output,
        image_keys.reshape(512, D),
        image_values.reshape(512, D),
    )
    return pl.pallas_call(
        emit,
        out_shape=tuple(jax.ShapeDtypeStruct(shape, BF16) for shape in shapes),
        in_specs=[vmem] * 3,
        out_specs=(vmem, vmem, vmem),
        name="emit",
    )(*[pltpu.with_memory_space_constraint(r, pltpu.VMEM) for r in results])


def solution(mesh):
    in_specs = (
        P(),
        P(),
        P("dp", None),
        P(),
        P(None, "patch"),
        P(None, "patch"),
        P(None, "patch"),
        P("patch", None),
        P("dp", None, "patch"),
        P("dp", None, "patch"),
        P(),
        P(),
        P(),
        P("dp", None, "patch", None),
        P("dp", None, "patch", None),
    )
    out_specs = (P("dp", None), P("dp", "patch"), P("dp", "patch"))
    return jax.shard_map(
        shards, mesh=mesh, in_specs=in_specs, out_specs=out_specs, check_vma=False
    )
```

```python
import jax
import jax.numpy as jnp
from jax import lax
from jax.experimental import pallas as pl
from jax.experimental.pallas import tpu as pltpu
from jax.sharding import PartitionSpec as P

MESH = pl.DeviceIdType.MESH
F32 = jnp.float32
BF16 = jnp.bfloat16

D = 1024
CHUNKS = 8
BEAMS = 4
IMAGES = 16
ROWS = BEAMS * IMAGES
DP = 32
PATCH = 8
PLANE = 32
SLAB = 1000
LEN = 128
SPOTS = 32
NEG = -1e30
NT = (((1,), (1,)), ((), ()))


def dot(a, b):
    return jnp.dot(a, b, preferred_element_type=F32)


def dot_nt(a, b):
    return lax.dot_general(a, b, NT, preferred_element_type=F32)


def tree(parts):
    while len(parts) > 1:
        parts = [a + b for a, b in zip(parts[::2], parts[1::2])] + (
            [parts[-1]] if len(parts) % 2 else []
        )
    return parts[0]


def hops(step, size):
    return min(step, size - step)


PARTNERS = sorted(
    [(dx, dy, dc) for dx in range(4) for dy in range(4) for dc in range(2) if dx + dy + dc],
    key=lambda t: -hops(t[0], 4) - hops(t[1], 4),
)
ACROSS = (2, 1, 3, 0)


def split_heads(x):
    lane = lax.broadcasted_iota(jnp.int32, x.shape, 1)
    low = jnp.where(lane < 64, x, 0.0)
    high = jnp.where(lane < 64, 0.0, x)
    return jnp.concatenate([low, high], axis=0).astype(BF16)


def join_heads(x):
    half = x.shape[0] // 2
    lane = lax.broadcasted_iota(jnp.int32, (half, 128), 1)
    return jnp.where(lane < 64, x[:half], x[half:])


def kernel(
    ids_hbm,
    parents_hbm,
    emb_ref,
    sgain_hbm,
    wq_ref,
    wk_ref,
    wv_ref,
    wo_ref,
    pk_ref,
    pv_ref,
    cgain_hbm,
    cq_ref,
    co_ref,
    ik_ref,
    iv_ref,
    hidden_ref,
    newk_ref,
    newv_ref,
    ids_ref,
    parents_ref,
    sgain_ref,
    cgain_ref,
    emb,
    wqkv,
    wo,
    pk,
    pv,
    cq,
    co,
    ik,
    iv,
    onehot,
    owned,
    r1,
    tokc,
    r2,
    tokf,
    part,
    partb,
    r4,
    row_f,
    prob,
    r5,
    probf,
    num,
    numb,
    r6,
    stat,
    r6s,
    hid,
    r7,
    hidf,
    load_sem,
    send_sem,
    recv_sem,
    ready,
):
    d = lax.axis_index("dp")
    p = lax.axis_index("patch")
    z, x = d // 4, d % 4
    y, c = p // 2, p % 2
    q = x * 8 + p
    zs = [lax.rem(z + k, 8) for k in range(8)]
    xs = [lax.rem(x + k, 4) for k in range(4)]
    ys = [lax.rem(y + k, 4) for k in range(4)]
    cs = [c, 1 - c]

    loads = []

    def load(src, dst):
        copy = pltpu.make_async_copy(src, dst, load_sem.at[len(loads)])
        copy.start()
        loads.append(copy)
        return copy

    emb[992:1024, :] = jnp.zeros((32, 128), BF16)
    l_ids = load(ids_hbm, ids_ref)
    l_emb = load(emb_ref.at[:, pl.ds(pl.multiple_of(p * 128, 128), 128)], emb.at[pl.ds(0, SLAB), :])

    barrier = pltpu.get_barrier_semaphore()

    def signal(sem, device):
        pl.semaphore_signal(sem, inc=1, device_id=device, device_id_type=MESH)

    for dz in range(1, 8):

        @pl.when(z + dz < 8)
        def _(dz=dz):
            for dx in ACROSS:
                signal(barrier, (zs[dz] * 4 + xs[dx], p))

    for dx, dy, dc in PARTNERS:
        signal(barrier, (z * 4 + xs[dx], ys[dy] * 2 + cs[dc]))

    row_f[...] = jnp.zeros((64, 128), F32)

    l_ids.wait()
    lane1024 = lax.broadcasted_iota(jnp.int32, (128, 1024), 1)
    for n in range(4):
        col = jnp.broadcast_to(ids_ref[n : n + 1, :], (128, 128)).T - d * SLAB
        wide = jnp.concatenate([col] * 8, axis=1)
        onehot[n * 128 : (n + 1) * 128, :] = jnp.where(wide == lane1024, 1.0, 0.0).astype(BF16)
    l_emb.wait()
    l_q = load(wq_ref, wqkv.at[:, 0:128])
    l_k = load(wk_ref, wqkv.at[:, 128:256])
    l_v = load(wv_ref, wqkv.at[:, 256:384])
    l_gain = load(sgain_hbm, sgain_ref)
    l_parents = load(parents_hbm, parents_ref)
    l_pk = load(pk_ref, pk)
    l_pv = load(pv_ref, pv)
    l_wo = load(wo_ref, wo)
    l_cgain = load(cgain_hbm, cgain_ref)
    l_cq = load(cq_ref, cq)
    l_ik = load(ik_ref, ik)
    l_iv = load(iv_ref, iv)
    l_co = load(co_ref, co)
    for n in range(4):
        rows = slice(n * 128, (n + 1) * 128)
        owned[rows, :] = dot(onehot[rows, :], emb[...]).astype(BF16)

    pl.semaphore_wait(barrier, (PLANE - 1) + 4 * z)
    for dz in range(1, 8):

        @pl.when(z + dz >= 8)
        def _(dz=dz):
            for dx in ACROSS:
                signal(ready.at[z], (zs[dz] * 4 + xs[dx], p))

    def await_bytes(ref, sem):
        pltpu.make_async_copy(ref, ref, sem).wait()

    def send1(dz, dx):
        to = zs[dz] * 4 + xs[dx]
        pltpu.make_async_remote_copy(
            src_ref=owned.at[pl.ds(pl.multiple_of(to * 16, 16), 16), :],
            dst_ref=r1.at[d],
            send_sem=send_sem.at[0],
            recv_sem=recv_sem.at[0],
            device_id=(to, p),
            device_id_type=MESH,
        ).start()

    for dz in (4, 3, 5, 2, 6, 1, 7):

        @pl.when(z + dz >= 8)
        def _(dz=dz):
            for dx in ACROSS:
                send1(dz, dx)

    for dx in ACROSS[:3]:
        send1(0, dx)
    for dz in range(1, 8):

        @pl.when(z + dz < 8)
        def _(dz=dz):
            pl.semaphore_wait(ready.at[zs[dz]], 4)
            for dx in ACROSS:
                send1(dz, dx)

    r1[d] = owned[pl.ds(pl.multiple_of(d * 16, 16), 16), :]
    await_bytes(r1.at[pl.ds(0, DP - 1)], recv_sem.at[0])
    chunk = tree([r1[s] for s in range(DP)])
    tokc[...] = chunk
    r2[q] = chunk

    def send_plane(src_of, dst, n):
        for dx, dy, dc in PARTNERS:
            to_x, to_p = xs[dx], ys[dy] * 2 + cs[dc]
            pltpu.make_async_remote_copy(
                src_ref=src_of(to_x, to_p),
                dst_ref=dst,
                send_sem=send_sem.at[n],
                recv_sem=recv_sem.at[n],
                device_id=(z * 4 + to_x, to_p),
                device_id_type=MESH,
            ).start()

    def await_plane(dst, n):
        await_bytes(dst.at[pl.ds(0, PLANE - 1)], recv_sem.at[n])

    send_plane(lambda to_x, to_p: tokc, r2.at[q], 1)
    l_q.wait()
    l_k.wait()
    l_v.wait()
    l_gain.wait()
    await_plane(r2, 1)

    toks = [
        jnp.concatenate([r2[b * 8 + j] for b in range(BEAMS)], axis=0).astype(F32)
        for j in range(CHUNKS)
    ]
    square = tree([t * t for t in toks])
    factor = lax.rsqrt(jnp.sum(square, axis=1, keepdims=True) * (1.0 / D) + 1e-06)
    sgain = sgain_ref[...].astype(F32)
    normed = jnp.concatenate(
        [(toks[j] * factor * sgain[j : j + 1, :]).astype(BF16) for j in range(CHUNKS)], axis=1
    )
    qkv = dot(normed, wqkv[...]).astype(BF16)
    new_q, new_k, new_v = (qkv[:, n * 128 : (n + 1) * 128].astype(F32) for n in range(3))
    queries = split_heads(new_q)
    own = jnp.sum(
        queries.astype(F32) * jnp.concatenate([new_k, new_k], axis=0), axis=1, keepdims=True
    )
    own = own * 0.125

    by_image = [pl.ds(i, 8, stride=16) for i in range(IMAGES)]
    hidf[...] = queries.astype(F32)
    l_pk.wait()
    parts = [
        dot_nt(hidf[by_image[i], :].astype(BF16), pk[i * LEN : (i + 1) * LEN, :])
        for i in range(IMAGES)
    ]
    for i in range(IMAGES):
        hidf[by_image[i], :] = parts[i]
    scores = hidf[...] * 0.125
    peak = jnp.maximum(jnp.max(scores, axis=1, keepdims=True), own)
    powers = jnp.exp(scores - peak)
    own_power = jnp.exp(own - peak)
    total = jnp.sum(powers, axis=1, keepdims=True) + own_power
    own_weight = own_power.astype(BF16).astype(F32)
    hidf[...] = powers
    l_pv.wait()
    parts = [
        dot(hidf[by_image[i], :].astype(BF16), pv[i * LEN : (i + 1) * LEN, :])
        for i in range(IMAGES)
    ]
    for i in range(IMAGES):
        hidf[by_image[i], :] = parts[i]
    context = hidf[...]
    context = (context + own_weight * jnp.concatenate([new_v, new_v], axis=0)) / total
    context = join_heads(context)
    l_parents.wait()
    pcol = jnp.broadcast_to(parents_ref[pl.ds(z // 2, 1), :], (128, 128)).T
    pcol = jnp.where(z % 2 == 0, pcol[:ROWS], pcol[ROWS:])
    context = jnp.where(pcol == x, context, 0.0).astype(BF16)

    l_wo.wait()
    projected = dot(context, wo[...])
    for j in range(CHUNKS):
        part[pl.ds(j, ROWS, stride=8), :] = projected[:, j * 128 : (j + 1) * 128]
    partb[...] = part[...].astype(BF16)
    mine = pl.ds(pl.multiple_of(q * 16, 16), 16)

    def part_of(to_x, to_p):
        return partb.at[pl.ds(pl.multiple_of((to_x * 8 + to_p) * 16, 16), 16), :]

    send_plane(part_of, r4.at[q], 2)
    r4[q] = partb[mine, :]
    hidf[0:ROWS, :] = new_k
    hidf[ROWS : 2 * ROWS, :] = new_v
    newk_ref[...] = hidf[pl.ds(pl.multiple_of(x * 16, 16), 16), :].astype(BF16)
    newv_ref[...] = hidf[pl.ds(pl.multiple_of(ROWS + x * 16, 16), 16), :].astype(BF16)
    for j in range(CHUNKS):
        tokf[pl.ds(j, 16, stride=8), :] = r2[x * 8 + j].astype(F32)
    l_cgain.wait()
    l_cq.wait()
    await_plane(r4, 2)
    middle = tree([r4[s].astype(F32) for s in range(PLANE)]) + tokf[pl.ds(pl.multiple_of(p * 16, 16), 16), :]

    cgain = cgain_ref[...].astype(F32)
    for r in range(2):
        row = middle[r * 8 : (r + 1) * 8, :]
        factor = lax.rsqrt(jnp.sum(row * row, keepdims=True) * (1.0 / D) + 1e-06)
        row_f[r * 8 : (r + 1) * 8, :] = row * factor * cgain

    def two_rows():
        return jnp.concatenate(
            [row_f[pl.ds(j, 8, stride=8), :] for j in range(CHUNKS)], axis=1
        ).astype(BF16)

    def back(value):
        for j in range(CHUNKS):
            row_f[pl.ds(j, 8, stride=8), :] = value[:, j * 128 : (j + 1) * 128]
        return row_f[0:16, :]

    mine_probe = back(dot(two_rows(), cq[...])).astype(BF16)
    prob[...] = mine_probe
    slot = p * 4 + x
    r5[slot] = mine_probe

    send_plane(lambda to_x, to_p: prob, r5.at[slot], 3)
    l_ik.wait()
    l_iv.wait()
    await_plane(r5, 3)

    probf[...] = r5[...].astype(F32).reshape(512, 128)
    units = [
        (slice(g * 128, (g + 1) * 128), slice(j * 128, (j + 1) * 128), pl.ds(g * 128 + j, 16, stride=8))
        for g in range(4)
        for j in range(CHUNKS)
    ]
    scores = jnp.concatenate(
        [dot_nt(split_heads(probf[rows, :]), ik[keys, block]) for keys, block, rows in units], axis=0
    )
    row = lax.broadcasted_iota(jnp.int32, scores.shape, 0)
    image = (row // 8 % 2) * 2 + row % 2
    same = image == lax.broadcasted_iota(jnp.int32, scores.shape, 1) // SPOTS
    scores = jnp.where(same, scores * 0.125, NEG)
    peak = jnp.max(scores, axis=1, keepdims=True)
    powers = jnp.exp(scores - peak)
    total = jnp.sum(powers, axis=1, keepdims=True)
    powers = powers.astype(BF16)
    lane = lax.broadcasted_iota(jnp.int32, (16, 128), 1)
    for g in range(4):
        stats = jnp.zeros((16, 128), F32)
        for j in range(CHUNKS):
            for h in range(2):
                at = (g * CHUNKS + j) * 32 + h * 16
                stats = jnp.where(lane == h * 8 + j, peak[at : at + 16], stats)
                stats = jnp.where(lane == 16 + h * 8 + j, total[at : at + 16], stats)
        stat[g * 16 : (g + 1) * 16, :] = stats
    def stat_of(to_x, to_p):
        return stat.at[pl.ds(pl.multiple_of((to_p * 4 + to_x) * 2, 2), 2), :]

    send_plane(stat_of, r6s.at[q], 5)
    for n, (keys, block, rows) in enumerate(units):
        num[rows, :] = join_heads(dot(powers[n * 32 : (n + 1) * 32], iv[keys, block]))
    numb[...] = num[...].astype(BF16)

    def num_of(to_x, to_p):
        return numb.at[pl.ds(pl.multiple_of((to_p * 4 + to_x) * 16, 16), 16), :]

    send_plane(num_of, r6.at[q], 4)
    r6[q] = numb[pl.ds(pl.multiple_of(slot * 16, 16), 16), :]
    r6s[q] = stat[pl.ds(pl.multiple_of(slot * 2, 2), 2), :]
    l_co.wait()
    await_plane(r6s, 5)
    stats = jnp.concatenate(
        [r6s[...].reshape(64, 128), jnp.zeros((64, 128), F32)], axis=0
    ).T
    lane8 = lax.broadcasted_iota(jnp.int32, (8, 128), 1)
    shares = []
    for r in range(2):
        valid = (lane8 < 64) & (lane8 % 2 == r)
        pair = []
        for h in range(2):
            peaks = jnp.where(valid, stats[h * 8 : (h + 1) * 8, :], NEG)
            totals = stats[16 + h * 8 : 16 + (h + 1) * 8, :]
            scale = jnp.where(valid, jnp.exp(peaks - jnp.max(peaks, axis=1, keepdims=True)), 0.0)
            pair.append((scale, jnp.sum(scale * totals, axis=1, keepdims=True)))
        shares.append(pair)
    await_plane(r6, 4)
    low = lane8 < 64
    for r in range(2):
        (scale0, total0), (scale1, total1) = shares[r]
        terms = []
        for s in range(PLANE):
            at = slice(2 * s + r, 2 * s + r + 1)
            scale = jnp.where(low, scale0[:, at], scale1[:, at])
            terms.append(r6[s].astype(F32)[r * 8 : (r + 1) * 8, :] * scale)
        row_f[r * 8 : (r + 1) * 8, :] = tree(terms) / jnp.where(low, total0, total1)
    final = (back(dot(two_rows(), co[...])) + middle).astype(BF16)
    hid[...] = final
    r7[p] = final

    for dx, dy, dc in PARTNERS:
        if dx == 0:
            pltpu.make_async_remote_copy(
                src_ref=hid,
                dst_ref=r7.at[p],
                send_sem=send_sem.at[6],
                recv_sem=recv_sem.at[6],
                device_id=(d, ys[dy] * 2 + cs[dc]),
                device_id_type=MESH,
            ).start()
    for n, ref in enumerate((r1, r2, r4, r5, r6, r6s)):
        await_bytes(ref.at[pl.ds(0, 31)], send_sem.at[n])
    await_bytes(r7.at[pl.ds(0, PATCH - 1)], recv_sem.at[6])
    hidf[...] = r7[...].astype(F32).reshape(128, 128)
    for j in range(CHUNKS):
        hidden_ref[:, j * 128 : (j + 1) * 128] = hidf[pl.ds(j, 16, stride=8), :].astype(BF16)
    await_bytes(r7.at[pl.ds(0, PATCH - 1)], send_sem.at[6])


def emit(hidden, new_k, new_v, hidden_ref, newk_ref, newv_ref):
    hidden_ref[...] = hidden[...]
    newk_ref[...] = new_k[...]
    newv_ref[...] = new_v[...]


def shards(
    token_ids,
    parents,
    embedding,
    self_gain,
    query_weight,
    key_weight,
    value_weight,
    output_weight,
    past_keys,
    past_values,
    cross_gain,
    cross_query,
    cross_output,
    image_keys,
    image_values,
):
    vmem = pl.BlockSpec(memory_space=pltpu.VMEM)
    hbm = pl.BlockSpec(memory_space=pl.ANY)
    shapes = ((16, D), (16, 128), (16, 128))
    results = pl.pallas_call(
        kernel,
        out_shape=tuple(pltpu.VMEM(shape, BF16) for shape in shapes),
        in_specs=[hbm] * 15,
        out_specs=(vmem, vmem, vmem),
        scratch_shapes=[
            pltpu.VMEM((4, 128), jnp.int32),
            pltpu.VMEM((4, 128), jnp.int32),
            pltpu.VMEM((8, 128), BF16),
            pltpu.VMEM((8, 128), BF16),
            pltpu.VMEM((1024, 128), BF16),
            pltpu.VMEM((D, 384), BF16),
            pltpu.VMEM((128, D), BF16),
            pltpu.VMEM((2048, 128), BF16),
            pltpu.VMEM((2048, 128), BF16),
            pltpu.VMEM((D, D), BF16),
            pltpu.VMEM((D, D), BF16),
            pltpu.VMEM((512, D), BF16),
            pltpu.VMEM((512, D), BF16),
            pltpu.VMEM((512, D), BF16),
            pltpu.VMEM((512, 128), BF16),
            pltpu.VMEM((DP, 16, 128), BF16),
            pltpu.VMEM((16, 128), BF16),
            pltpu.VMEM((PLANE, 16, 128), BF16),
            pltpu.VMEM((128, 128), F32),
            pltpu.VMEM((512, 128), F32),
            pltpu.VMEM((512, 128), BF16),
            pltpu.VMEM((PLANE, 16, 128), BF16),
            pltpu.VMEM((64, 128), F32),
            pltpu.VMEM((16, 128), BF16),
            pltpu.VMEM((PLANE, 16, 128), BF16),
            pltpu.VMEM((512, 128), F32),
            pltpu.VMEM((512, 128), F32),
            pltpu.VMEM((512, 128), BF16),
            pltpu.VMEM((PLANE, 16, 128), BF16),
            pltpu.VMEM((ROWS, 128), F32),
            pltpu.VMEM((PLANE, 2, 128), F32),
            pltpu.VMEM((16, 128), BF16),
            pltpu.VMEM((PATCH, 16, 128), BF16),
            pltpu.VMEM((128, 128), F32),
            pltpu.SemaphoreType.DMA((15,)),
            pltpu.SemaphoreType.DMA((7,)),
            pltpu.SemaphoreType.DMA((7,)),
            pltpu.SemaphoreType.REGULAR((8,)),
        ],
        compiler_params=pltpu.CompilerParams(collective_id=0, has_side_effects=True),
        name="step",
    )(
        token_ids.reshape(4, 128),
        parents.reshape(4, 128),
        embedding,
        self_gain.reshape(8, 128),
        query_weight,
        key_weight,
        value_weight,
        output_weight,
        past_keys.reshape(2048, 128),
        past_values.reshape(2048, 128),
        cross_gain.reshape(8, 128),
        cross_query,
        cross_output,
        image_keys.reshape(512, D),
        image_values.reshape(512, D),
    )
    return pl.pallas_call(
        emit,
        out_shape=tuple(jax.ShapeDtypeStruct(shape, BF16) for shape in shapes),
        in_specs=[vmem] * 3,
        out_specs=(vmem, vmem, vmem),
        name="emit",
    )(*[pltpu.with_memory_space_constraint(r, pltpu.VMEM) for r in results])


def solution(mesh):
    in_specs = (
        P(),
        P(),
        P("dp", None),
        P(),
        P(None, "patch"),
        P(None, "patch"),
        P(None, "patch"),
        P("patch", None),
        P("dp", None, "patch"),
        P("dp", None, "patch"),
        P(),
        P(),
        P(),
        P("dp", None, "patch", None),
        P("dp", None, "patch", None),
    )
    out_specs = (P("dp", None), P("dp", "patch"), P("dp", "patch"))
    return jax.shard_map(
        shards, mesh=mesh, in_specs=in_specs, out_specs=out_specs, check_vma=False
    )
```
